256 devices in a mesh: dp: 32 (over x, z), vocab: 8 (over y, core).
Axes of the slice: x: 4, y: 4, z: 8, core: 2. Of those that a mesh axis runs over, the one named last changes fastest.
Arguments:
- hidden: bfloat16 [256, 14, 4096], P('dp', None, 'vocab'), may hold values from -400 to 400
- weight: bfloat16 [4096, 128256], P(None, ('dp', 'vocab')), may hold values from -0.09375 to 0.09375
- targets: int32 [256, 14], P('dp'), may hold values from 0 to 128255
- lengths: int32 [32, 8], P('dp'), may hold values from 1 to 14, 56 in all within a row
- rewards: int32 [32, 8], P('dp'), may hold values from -256 to 256
- arrival: int32 [256], replicated, may hold values from 0 to 255, each once
Outputs:
- token_logprobs: float32 [256, 14], P('dp')
- advantages: float32 [256], P('dp')
- weighted: float32 [256], P('dp')
The draws below stay inside these ranges and needn't reach their ends.
Inputs may be any that keep to these rules, and one draw needn't show every extreme that they name: The lengths of one device's 8 completions sum to exactly 56, and one of them is 14. `arrival`: every completion number appears once; completion p * 8 + j is sample j of prompt p.
All inputs are finite; a program needn't handle non-finite values.
Results may differ from the reference program's by a relative error of at most 0.0003.
Values may be sent and summed in bfloat16 or wider, within the bound.
No kernel may reach another device: no remote copies, remote signals or barrier semaphores. Data moves between devices by JAX's collectives and lax.ppermute only.
A program may use at most 192 MiB of HBM per device.

```python
import math
import jax
import jax.numpy as jnp
import numpy as np
from jax import lax

D = 4096
SAMPLES = 8
BLOCK = 14
CPL_DEV = 8
LIVE_DEV = 56
COMPL = 256
ROWS = 3584
VOCAB = 128256
N_DP = 32


def draw_hidden(key, part):
    first = jax.random.fold_in(key, 0)
    base = jnp.clip(jax.random.normal(first, (COMPL, BLOCK, D), jnp.float32), -6.0, 6.0)
    factor = 3.0
    return (base * factor).astype(jnp.bfloat16)


def with_ends(values, rng, low, largest):
    shape = values.shape
    index_at = [jax.random.randint(jax.random.fold_in(rng, axis), (), 0, shape[axis]) for axis in range(len(shape))]
    values = values.at[tuple(index_at)].set(low)
    longest = shape.index(max(shape))
    index_at[longest] = (index_at[longest] + 1) % shape[longest]
    return values.at[tuple(index_at)].set(largest)


def levels(rng, extent, cuts, smallest, top_value):
    def one(position, parts):
        heights = jax.random.uniform(jax.random.fold_in(jax.random.fold_in(rng, 6), position), (parts,), jnp.float32, smallest / len(cuts), top_value / len(cuts))
        return jnp.repeat(jnp.exp(heights), extent[position] // parts).reshape((-1,) + (1,) * (len(extent) - position - 1))

    loudness = one(*cuts[0])
    for cut in cuts[1:]:
        loudness = loudness * one(*cut)
    return loudness


def profile(number_of, total, limit, skew):
    portions = [(1 << 20) // math.isqrt(standing ** skew) + 1 for standing in range(2, number_of + 1)]
    rest, given = total - limit - (number_of - 1), [1] * (number_of - 1)
    while rest > 0:
        free = [i for i in range(number_of - 1) if given[i] < limit]
        pool, budget = sum([portions[i] for i in free]), rest
        for i in free:
            extra = min(limit - given[i], max(1, budget * portions[i] // pool), rest)
            given[i] = given[i] + extra
            rest = rest - extra
    return np.array([limit] + given)


def ragged_sizes(rng, count, total, bound, lean):
    if count == 2:
        one = jax.random.randint(rng, (), max(1, total - bound), min(bound, total - 1) + 1)
        return jnp.stack([one, total - one])
    sizes = jnp.asarray(profile(count, total, bound, lean), jnp.int32)
    pairs = (count - 1) // 2
    donor, sink = sizes[1:1 + 2 * pairs:2], sizes[2:2 + 2 * pairs:2]
    slack = jnp.minimum(donor - 1, bound - sink)
    shifted = jax.random.randint(jax.random.fold_in(rng, 1), (pairs,), 0, 1 << 20) % (slack + 1)
    sizes = sizes.at[1:1 + 2 * pairs:2].set(donor - shifted).at[2:2 + 2 * pairs:2].set(sink + shifted)
    return sizes[jax.random.permutation(jax.random.fold_in(rng, 2), count)]


def centred(stream_key, shape, scale, limit, cuts=(), held_as=jnp.bfloat16):
    level = levels(stream_key, shape, cuts, -0.22, 0.18) if cuts else 1.0
    drawn = jax.random.normal(stream_key, shape, jnp.float32) * scale * level
    return jnp.minimum(jnp.maximum(drawn, -limit), limit).astype(held_as)


def setup_inputs(seed: int = 0) -> dict:
    splits = jax.random.split(jax.random.key(seed), 7)
    return {
        "hidden": draw_hidden(jax.random.fold_in(splits[6], 71), 0),
        "weight": centred(splits[1], (D, VOCAB), D ** -0.5, 0.09375, ((1, 256),)),
        "targets": with_ends(jax.random.randint(splits[2], (COMPL, BLOCK), 0, VOCAB), jax.random.fold_in(splits[2], 1), 0, VOCAB - 1).astype(jnp.int32),
        "lengths": jax.vmap(lambda own: ragged_sizes(own, CPL_DEV, LIVE_DEV, BLOCK, 2))(jax.random.split(splits[3], N_DP)).reshape((N_DP, CPL_DEV)).astype(jnp.int32),
        "rewards": with_ends(jax.random.randint(splits[4], (N_DP, CPL_DEV), -256, 257), jax.random.fold_in(splits[4], 1), -256, 256).astype(jnp.int32),
        "arrival": jax.random.permutation(splits[5], COMPL).astype(jnp.int32),
    }


reward_unit = 1.0 / 64.0


def reference(hidden, weight, targets, lengths, rewards, arrival):
    row_states = hidden.reshape(ROWS, D)
    token_ids = targets.reshape(ROWS)
    column_span = VOCAB // N_DP

    def absorb(carried, block_index):
        highest, totals = carried
        columns = lax.dynamic_slice_in_dim(weight, block_index * column_span, column_span, 1)
        logits = jnp.dot(row_states, columns, preferred_element_type=jnp.float32)
        block_high = jnp.max(logits, axis=1)
        block_total = jnp.sum(jnp.exp(logits - block_high[:, None]), axis=1)
        joined = jnp.maximum(highest, block_high)
        totals = totals * jnp.exp(highest - joined) + block_total * jnp.exp(block_high - joined)
        return (joined, totals), None

    start = (jnp.full((ROWS,), -1e30, jnp.float32), jnp.zeros((ROWS,), jnp.float32))
    (highest, totals), _ = lax.scan(absorb, start, jnp.arange(N_DP, dtype=jnp.int32))
    chosen = jnp.take(weight, token_ids, axis=1)
    picked = jnp.sum(row_states.astype(jnp.float32) * chosen.T.astype(jnp.float32), axis=1)
    slot_lengths = lengths.reshape(COMPL)
    usable = jnp.arange(BLOCK, dtype=jnp.int32)[None, :] < slot_lengths[:, None]
    slot_logprob = jnp.where(usable, (picked - highest - jnp.log(totals)).reshape(COMPL, BLOCK), 0.0)
    token_logprobs = jnp.zeros((COMPL, BLOCK), jnp.float32).at[arrival].set(slot_logprob)
    reward = jnp.zeros((COMPL,), jnp.float32).at[arrival].set(rewards.reshape(COMPL).astype(jnp.float32) * reward_unit)
    length = jnp.zeros((COMPL,), jnp.float32).at[arrival].set(slot_lengths.astype(jnp.float32))
    group = jnp.sum(reward.reshape(COMPL // SAMPLES, SAMPLES), axis=1)
    advantages = reward - (jnp.repeat(group, SAMPLES) - reward) / (SAMPLES - 1.0)
    weighted = advantages * jnp.sum(token_logprobs, axis=1) / length
    return token_logprobs, advantages, weighted
```

```python
import jax
import jax.numpy as jnp
from jax import lax
from jax.experimental import pallas as pl
from jax.experimental.pallas import tpu as pltpu
from jax.sharding import Mesh
from jax.sharding import PartitionSpec as P

SAMPLES = 8
DP = ("x", "z")
VOCAB = ("y", "c")
REWARD_UNIT = 1.0 / 64.0
NX, NZ, NY, NC = 4, 8, 4, 2
HALF = 28
META = 8
ROWS = 4 * HALF


def shift(value, axis, by):
    size = lax.axis_size(axis)
    return lax.ppermute(value, axis, [(i, (i + by) % size) for i in range(size)])


def packed_messages(hidden, targets, lengths, rewards):
    slots, window, width = hidden.shape
    live = 2 * HALF
    position = lax.iota(jnp.int32, window)
    mask = (position[None, :] < lengths[0][:, None]).reshape(slots * window)
    counting = mask.astype(jnp.int32)
    place = jnp.cumsum(counting) - counting
    chooser = (place[None, :] == lax.iota(jnp.int32, live)[:, None]) & mask[None, :]
    rows = jnp.dot(
        chooser.astype(jnp.bfloat16),
        hidden.reshape(slots * window, width),
        preferred_element_type=jnp.float32,
    ).astype(jnp.bfloat16)
    ids = jnp.sum(jnp.where(chooser, targets.reshape(slots * window)[None, :], 0), axis=1)
    digits = jnp.stack([ids % 256, ids // 256 % 256, ids // 65536], 0)
    digits = digits.reshape(3, NC, HALF).transpose(1, 0, 2).reshape(NC, 3 * HALF)
    both = jnp.concatenate([lengths, rewards], 1)
    meta = jnp.concatenate([digits, jnp.broadcast_to(both, (NC, both.shape[1]))], 1)
    meta = meta.astype(jnp.float32).astype(jnp.bfloat16)[:, None, :]
    meta = jnp.pad(meta, ((0, 0), (0, 3), (0, width - meta.shape[2])))
    return jnp.concatenate([rows.reshape(NC, HALF, width), meta], 1)


def gathered_axis_pair(own, first, last):
    up, down = shift(own, first, 1), shift(own, first, -1)
    half = own.shape[0] // 16 * 8
    low, high = shift(up[:half], first, 1), shift(down[half:], first, -1)
    line = jnp.concatenate([own, up, down, low, high], 0)
    return line


def gathered_last(line, last):
    up, down = shift(line, last, 1), shift(line, last, -1)
    half = line.shape[0] // 2
    low, high = shift(up[:half], last, 1), shift(down[half:], last, -1)
    return line, up, down, low, high


OFFSETS = (0, -1, 1, 2)


def head_kernel(at, ids, a0, a1, a2, a3l, a3h, b0, b1, b2, b3l, b3h, w_own, w_other, out, acc):
    x, y, own_first, other_first = at[0], at[1], at[2], at[3]
    wide = 4 * ROWS
    shard = w_own.shape[0]
    out[...] = jnp.zeros_like(out)

    def dot(w, block, k_at):
        k = block.shape[1]
        return lax.dot_general(
            w[:, pl.ds(pl.multiple_of(k_at, k), k)],
            block,
            (((1,), (1,)), ((), ())),
            preferred_element_type=jnp.float32,
        )

    def k_of(j):
        return (y + OFFSETS[j] + NY) % NY * 1024

    def stats(colour, blocks_of, rows):
        for w, ref in enumerate((w_own, w_other)):
            acc[w, :, :rows] = blocks_of(ref)
        own, other = acc[0, :, :rows], acc[1, :, :rows]
        top = jnp.maximum(jnp.max(own, 0, keepdims=True), jnp.max(other, 0, keepdims=True))
        total = jnp.sum(jnp.exp(own - top), 0, keepdims=True) + jnp.sum(
            jnp.exp(other - top), 0, keepdims=True
        )
        column = lax.broadcasted_iota(jnp.int32, (shard, rows), 0)
        wanted = ids[colour : colour + 1, :rows]
        hit = jnp.sum(jnp.where(column == wanted - own_first, own, 0.0), 0, keepdims=True)
        hit += jnp.sum(jnp.where(column == wanted - other_first, other, 0.0), 0, keepdims=True)
        return top + jnp.log(total), hit

    piece = ROWS + META

    def colour0(ref):
        total = None
        for j, pieces in enumerate(((a0,), (a1,), (a2,), (a3l, a3h))):
            block = jnp.concatenate([p[...] for p in pieces], 0)
            term = dot(ref, block, k_of(j))
            total = term if total is None else total + term
        return total

    lse, hit = stats(0, colour0, 4 * piece)
    for i in range(4):
        x_at = (x + OFFSETS[i] + NX) % NX
        out[pl.ds(x_at, 1), :ROWS] = lse[:, i * piece : i * piece + ROWS]
        out[pl.ds(8 + x_at, 1), :ROWS] = hit[:, i * piece : i * piece + ROWS]

    def colour1(ref):
        total = None
        for j in range(4):
            rows = [b[j * ROWS : (j + 1) * ROWS, :] for b in (b0, b1, b2)]
            split = b3l if j < 2 else b3h
            rows.append(split[j % 2 * ROWS : (j % 2 + 1) * ROWS, :])
            term = dot(ref, jnp.concatenate(rows, 0), k_of(j))
            total = term if total is None else total + term
        return total

    lse, hit = stats(1, colour1, wide)
    for i in range(4):
        x_at = (x + OFFSETS[i] + NX) % NX
        out[pl.ds(4 + x_at, 1), :ROWS] = lse[:, i * ROWS : (i + 1) * ROWS]
        out[pl.ds(12 + x_at, 1), :ROWS] = hit[:, i * ROWS : (i + 1) * ROWS]


def merged(parts):
    lse, hit = parts[:, :8], parts[:, 8:]
    top = jnp.max(lse, axis=0)
    lse = top + jnp.log(jnp.sum(jnp.exp(lse - top), axis=0))
    return jnp.concatenate([lse, jnp.sum(hit, axis=0)], 0)


def to_all(value, axes):
    size = lax.axis_size(axes)
    return lax.all_to_all(jnp.broadcast_to(value[None], (size, *value.shape)), axes, 0, 0, tiled=True)


def local(hidden, weight, targets, lengths, rewards, arrival):
    slots, window, width = hidden.shape
    shard = weight.shape[1]
    x, z, y, c = (lax.axis_index(a) for a in ("x", "z", "y", "c"))
    swapped = shift(weight, "c", 1)
    messages = packed_messages(hidden, targets, lengths, rewards)
    sent = jnp.broadcast_to(messages[None], (NZ, *messages.shape)).reshape(NZ * NC, 32, width)
    got = lax.all_to_all(sent, ("z", "c"), 0, 0, tiled=True).reshape(NZ, NC, 32, width)
    block = got[:, :, :HALF].transpose(0, 2, 1, 3).reshape(NZ * HALF, NC * width)
    meta = jnp.pad(got[:, 0, HALF], ((0, 0), (0, width)))
    line0 = gathered_axis_pair(jnp.concatenate([block[:ROWS], meta], 0), "x", "y")
    line1 = gathered_axis_pair(block[ROWS:], "y", "x")
    a = gathered_last(line0, "y")
    b = gathered_last(line1, "x")

    piece = ROWS + META
    metas = line0.reshape(4, piece, NC * width)[:, ROWS:, :128].astype(jnp.float32)
    whole = metas.astype(jnp.int32)
    digits = whole[:, :, : 3 * HALF].reshape(4, NZ, 3, HALF)
    ids = digits[:, :, 0] + 256 * digits[:, :, 1] + 65536 * digits[:, :, 2]
    ids0 = jnp.pad(ids[:, :4].reshape(4, ROWS), ((0, 0), (0, META)), constant_values=-1)
    ids1 = jnp.pad(ids[:, 4:].reshape(1, 4 * ROWS), ((0, 0), (0, 4 * META)), constant_values=-1)
    ids_all = jnp.concatenate([ids0.reshape(1, 4 * piece), ids1], 0)
    ids_all = jnp.pad(ids_all, ((0, 6), (0, 0)), constant_values=-1)

    dp = x * NZ + z
    base = (dp * NY + y) * NC
    at = jnp.stack([x, y, (base + c) * shard, (base + 1 - c) * shard]).astype(jnp.int32)
    vmem = pl.BlockSpec(memory_space=pltpu.VMEM)
    partial = pl.pallas_call(
        head_kernel,
        out_shape=jax.ShapeDtypeStruct((16, 128), jnp.float32),
        in_specs=[pl.BlockSpec(memory_space=pltpu.SMEM)] + [vmem] * 13,
        out_specs=vmem,
        scratch_shapes=[pltpu.VMEM((2, shard, 4 * piece), jnp.float32)],
        compiler_params=pltpu.CompilerParams(vmem_limit_bytes=56 * 2**20),
    )(at, ids_all, *a, *b, weight.T, swapped.T)

    stats = merged(to_all(partial, ("x", "y")))
    stats = merged(to_all(stats, "z"))
    logprob = stats[8:] - stats[:8]
    other = shift(logprob, "c", 1)
    flat = jnp.where(c == 0, jnp.stack([logprob, other]), jnp.stack([other, logprob])).reshape(-1)

    order = (lax.iota(jnp.int32, 4) - x + NX) % NX
    relative = jnp.array([0, 2, 3, 1], jnp.int32)[order]
    tables = jnp.sum(
        jnp.where(
            (relative[:, None] == lax.iota(jnp.int32, 4)[None, :])[:, :, None, None],
            whole[None, :, :, 3 * HALF : 3 * HALF + 16],
            0,
        ),
        axis=1,
    ).reshape(NX * NZ, 16)
    all_lengths, all_rewards = tables[:, :8], tables[:, 8:]
    total = NX * NZ * slots
    slot_ids = lax.iota(jnp.int32, total)
    mine = lax.iota(jnp.int32, slots) + dp * slots
    matching = arrival[None, :] == mine[:, None]

    def lookup(table):
        return jnp.sum(jnp.where(matching, table.reshape(total)[None, :], 0), axis=1)

    slot_of = lookup(slot_ids)
    length_of = lookup(all_lengths)
    reward_of = lookup(all_rewards).astype(jnp.float32) * REWARD_UNIT
    offset_of = lookup(jnp.cumsum(all_lengths, axis=1) - all_lengths)
    group = slot_of // slots
    line = offset_of[:, None] + lax.iota(jnp.int32, window)[None, :]
    usable = lax.iota(jnp.int32, window)[None, :] < length_of[:, None]
    gx, gz = group // NZ, group % NZ
    place = (gz // 4 * 4 + gx) * 128 + gz % 4 * HALF
    source = jnp.where(usable, place[:, None] + line // HALF * 1024 + line % HALF, 0)
    token_logprobs = jnp.where(usable, flat[source], 0.0)
    groups = jnp.sum(reward_of.reshape(slots // SAMPLES, SAMPLES), axis=1)
    advantages = reward_of - (jnp.repeat(groups, SAMPLES) - reward_of) / (SAMPLES - 1.0)
    weighted = advantages * jnp.sum(token_logprobs, axis=1) / length_of.astype(jnp.float32)
    return token_logprobs, advantages, weighted


def solution(mesh):
    finer = Mesh(mesh.devices.reshape(NX, NZ, NY, NC), ("x", "z", "y", "c"))
    every = ("x", "z", "y", "c")
    placed = (P(DP, None, VOCAB), P(None, every), P(DP, None), P(DP, None), P(DP, None), P())
    return jax.shard_map(
        local, mesh=finer, in_specs=placed, out_specs=(P(DP, None), P(DP), P(DP)), check_vma=False
    )
```

```python
import jax
import jax.numpy as jnp
from jax import lax
from jax.experimental import pallas as pl
from jax.experimental.pallas import tpu as pltpu
from jax.sharding import Mesh
from jax.sharding import PartitionSpec as P

SAMPLES = 8
DP = ("x", "z")
VOCAB = ("y", "c")
REWARD_UNIT = 1.0 / 64.0
NX, NZ, NY, NC = 4, 8, 4, 2
SLOTS, WINDOW, WIDTH = 8, 14, 512
HALF = 28
MSG = 32
ROWS = NZ * HALF
META = NZ
TALL = ROWS + META
OFFSETS = (0, -1, 1, 2)
F32 = jnp.float32
BF16 = jnp.bfloat16
VMEM = pl.BlockSpec(memory_space=pltpu.VMEM)
SMEM = pl.BlockSpec(memory_space=pltpu.SMEM)


def params(mib=32):
    return pltpu.CompilerParams(vmem_limit_bytes=mib * 2**20)


def shift(value, axis, by):
    size = lax.axis_size(axis)
    return lax.ppermute(value, axis, [(i, (i + by) % size) for i in range(size)])


def pack_kernel(lengths, both, hidden, targets, out):
    ends, offsets = [], []
    at = jnp.int32(0)
    for g in range(SLOTS):
        offsets.append(at)
        at = at + lengths[0, g]
    row = lax.broadcasted_iota(jnp.int32, (MSG, WINDOW), 0)
    step = lax.broadcasted_iota(jnp.int32, (MSG, WINDOW), 1)
    wanted = targets[...]
    digits = [(wanted & 255), (wanted >> 8) & 255, wanted >> 16]
    lane_both = jnp.concatenate(
        [both[...].astype(F32), jnp.zeros((1, 128 - 2 * SLOTS), F32)], axis=1
    )
    out_row = lax.broadcasted_iota(jnp.int32, (MSG, WIDTH), 0)
    for half in range(NC):
        rows = jnp.zeros((MSG, WIDTH), F32)
        ids = jnp.zeros((8, MSG), F32)
        for g in range(SLOTS):
            here = (row + half * HALF == offsets[g] + step) & (step < lengths[0, g]) & (row < HALF)
            chooser = jnp.where(here, 1.0, 0.0).astype(BF16)
            rows += jnp.dot(chooser, hidden[g], preferred_element_type=F32)
            three = jnp.concatenate(
                [d[g : g + 1, :] for d in digits] + [jnp.zeros((5, WINDOW), jnp.int32)], axis=0
            )
            ids += lax.dot_general(
                three.astype(F32).astype(BF16),
                chooser,
                (((1,), (1,)), ((), ())),
                preferred_element_type=F32,
            )
        pad = jnp.zeros((1, 128 - MSG), F32)
        meta = jnp.concatenate(
            [ids[0:1], pad, ids[1:2], pad, ids[2:3], pad, lane_both], axis=1
        )
        message = jnp.where(out_row == HALF, meta, rows).astype(BF16)
        for z in range(NZ):
            out[z * NC + half] = message


def unpack_kernel(got, first, second):
    for core, out in enumerate((first, second)):
        pieces = [got[z * NC + core].astype(F32)[:HALF] for z in range(NZ)]
        if core == 0:
            pieces += [got[z * NC].astype(F32)[HALF : HALF + 1] for z in range(NZ)]
        out[...] = jnp.concatenate(pieces, axis=0).astype(BF16)


def join_kernel(*refs):
    out = refs[-1]
    at = 0
    for ref in refs[:-1]:
        out[at : at + ref.shape[0]] = ref[...]
        at += ref.shape[0]


def join(*parts):
    rows = sum(p.shape[0] for p in parts)
    return pl.pallas_call(
        join_kernel,
        out_shape=jax.ShapeDtypeStruct((rows, parts[0].shape[1]), BF16),
        in_specs=[VMEM] * len(parts),
        out_specs=VMEM,
        compiler_params=params(),
    )(*parts)


def gathered_line(own, axis):
    up, down = shift(own, axis, 1), shift(own, axis, -1)
    half = own.shape[0] // 32 * 16
    low, high = shift(up[:half], axis, 1), shift(down[half:], axis, -1)
    return join(own, up), join(down, low, high)


def gathered_plane(line, axis):
    one, two = line
    up1, down1 = shift(one, axis, 1), shift(one, axis, -1)
    up2, down2 = shift(two, axis, 1), shift(two, axis, -1)
    far1, far2 = shift(up1, axis, 1), shift(down2, axis, -1)
    return (one, two), (up1, up2), (down1, down2), (far1, far2)


def product(w, block, k):
    return lax.dot_general(
        w[:, pl.ds(pl.multiple_of(k, WIDTH), WIDTH)],
        block,
        (((1,), (1,)), ((), ())),
        preferred_element_type=F32,
    )


def matmul_kernel(which, first, last):
    def kernel(at, *refs):
        y = at[0]
        n = 2 * len(which)
        a, b = refs[:n], refs[n : 2 * n]
        ws = refs[2 * n : 2 * n + 2]
        rest = refs[2 * n + 2 :]
        if first:
            (acc,) = rest
            before = None
        else:
            before, acc = rest[0], rest[-1]

        def k_of(j, core):
            return ((y + OFFSETS[j] + NY) % NY * NC + core) * WIDTH

        for w, ref in enumerate(ws):
            for i in range(NX):
                terms = []
                for p, j in enumerate(which):
                    source = a[2 * p + i // 2]
                    lo = i % 2 * TALL
                    terms.append(product(ref, source[lo : lo + ROWS, :], k_of(j, 0)))
                if i in which:
                    p = which.index(i)
                    for j in range(NY):
                        source = b[2 * p + j // 2]
                        lo = j % 2 * ROWS
                        terms.append(product(ref, source[lo : lo + ROWS, :], k_of(j, 1)))
                total = terms[0]
                for t in terms[1:]:
                    total = total + t
                if not first:
                    total = total + before[w, i]
                acc[w, i] = total
        if last:
            statistics(at, rest[1], acc, rest[2])

    return kernel


def statistics(at, ids, acc, out):
    x = at[1]
    shard = acc.shape[2]
    out[...] = jnp.zeros_like(out)
    column = lax.broadcasted_iota(jnp.int32, (shard, ROWS), 0)
    for i in range(NX):
        own, other = acc[0, i], acc[1, i]
        top = jnp.maximum(jnp.max(own, 0, keepdims=True), jnp.max(other, 0, keepdims=True))
        total = jnp.sum(jnp.exp(own - top), 0, keepdims=True) + jnp.sum(
            jnp.exp(other - top), 0, keepdims=True
        )
        wanted = ids[i : i + 1, :ROWS]
        hit = jnp.sum(jnp.where(column == wanted - at[2], own, 0.0), 0, keepdims=True)
        hit += jnp.sum(jnp.where(column == wanted - at[3], other, 0.0), 0, keepdims=True)
        x_at = (x + OFFSETS[i] + NX) % NX
        out[pl.ds(x_at, 1), :ROWS] = top + jnp.log(total)
        out[pl.ds(4 + x_at, 1), :ROWS] = hit


def head(at, plane0, plane1, weights, ids):
    shard = weights[0].shape[0]
    acc_shape = jax.ShapeDtypeStruct((2, NX, shard, ROWS), F32)

    def call(which, before=None, last=False):
        parts = [piece for j in which for piece in plane0[j]]
        parts += [piece for j in which for piece in plane1[j]]
        inputs = [at, *parts, *weights]
        first = before is None
        if not first:
            inputs.append(before)
        if last:
            inputs.append(ids)
        return pl.pallas_call(
            matmul_kernel(which, first, last),
            out_shape=jax.ShapeDtypeStruct((8, 256), F32) if last else acc_shape,
            in_specs=[SMEM] + [VMEM] * (len(inputs) - 1),
            out_specs=VMEM,
            scratch_shapes=[pltpu.VMEM(acc_shape.shape, F32)] if last else [],
            input_output_aliases={} if first or last else {len(inputs) - 1: 0},
            compiler_params=params(56),
        )(*inputs)

    acc = call((0,))
    acc = call((1, 2), acc)
    return call((3,), acc, True)


def merge_kernel(parts, out):
    lse, hit = parts[0, :4], parts[0, 4:]
    top = lse
    for k in range(1, parts.shape[0]):
        top = jnp.maximum(top, parts[k, :4])
        hit = hit + parts[k, 4:]
    total = jnp.zeros_like(top)
    for k in range(parts.shape[0]):
        total = total + jnp.exp(parts[k, :4] - top)
    out[:4] = top + jnp.log(total)
    out[4:] = hit


def merged(parts):
    return pl.pallas_call(
        merge_kernel,
        out_shape=jax.ShapeDtypeStruct(parts.shape[1:], F32),
        in_specs=[VMEM],
        out_specs=VMEM,
        compiler_params=params(),
    )(parts)


def to_all(value, axes):
    size = lax.axis_size(axes)
    return lax.all_to_all(jnp.broadcast_to(value[None], (size, *value.shape)), axes, 0, 0, tiled=True)


def local(hidden, weight, targets, lengths, rewards, arrival):
    shard = weight.shape[1]
    x, z, y, c = (lax.axis_index(a) for a in ("x", "z", "y", "c"))
    swapped = shift(weight, "c", 1)
    sent = pl.pallas_call(
        pack_kernel,
        out_shape=jax.ShapeDtypeStruct((NZ * NC, MSG, WIDTH), BF16),
        in_specs=[SMEM, VMEM, VMEM, VMEM],
        out_specs=VMEM,
        compiler_params=params(),
    )(lengths, jnp.concatenate([lengths, rewards], 1), hidden, targets)
    got = lax.all_to_all(sent, ("z", "c"), 0, 0, tiled=True)
    own0, own1 = pl.pallas_call(
        unpack_kernel,
        out_shape=[
            jax.ShapeDtypeStruct((TALL, WIDTH), BF16),
            jax.ShapeDtypeStruct((ROWS, WIDTH), BF16),
        ],
        in_specs=[VMEM],
        out_specs=[VMEM, VMEM],
        compiler_params=params(),
    )(got)
    line0, line1 = gathered_line(own0, "x"), gathered_line(own1, "y")
    plane0, plane1 = gathered_plane(line0, "y"), gathered_plane(line1, "x")

    metas = jnp.stack([line0[i // 2][i % 2 * TALL + ROWS : i % 2 * TALL + TALL] for i in range(NX)])
    whole = metas.astype(F32).astype(jnp.int32)
    ids = whole[:, :, :HALF] + 256 * whole[:, :, 128 : 128 + HALF] + 65536 * whole[:, :, 256 : 256 + HALF]
    ids = jnp.pad(ids.reshape(NX, ROWS), ((0, 4), (0, 0)), constant_values=-1)

    dp = x * NZ + z
    base = (dp * NY + y) * NC
    at = jnp.stack([y, x, (base + c) * shard, (base + 1 - c) * shard]).astype(jnp.int32)
    partial = head(at, plane0, plane1, (weight.T, swapped.T), ids)

    stats = merged(to_all(partial, ("x", "y")))
    last = to_all(stats, ("z", "c")).reshape(NZ, NC, 8, 256)
    tables = [merged(last[:, core]) for core in range(NC)]
    flat = jnp.stack([t[4:] - t[:4] for t in tables]).reshape(-1)

    order = (lax.iota(jnp.int32, NX) - x + NX) % NX
    relative = jnp.array([0, 2, 3, 1], jnp.int32)[order]
    per_slot = jnp.sum(
        jnp.where(
            (relative[:, None] == lax.iota(jnp.int32, NX)[None, :])[:, :, None, None],
            whole[None, :, :, 384 : 384 + 2 * SLOTS],
            0,
        ),
        axis=1,
    ).reshape(NX * NZ, 2 * SLOTS)
    all_lengths, all_rewards = per_slot[:, :SLOTS], per_slot[:, SLOTS:]
    count = NX * NZ * SLOTS
    slot_ids = lax.iota(jnp.int32, count)
    mine = lax.iota(jnp.int32, SLOTS) + dp * SLOTS
    matching = arrival[None, :] == mine[:, None]

    def lookup(table):
        return jnp.sum(jnp.where(matching, table.reshape(count)[None, :], 0), axis=1)

    slot_of = lookup(slot_ids)
    length_of = lookup(all_lengths)
    reward_of = lookup(all_rewards).astype(F32) * REWARD_UNIT
    offset_of = lookup(jnp.cumsum(all_lengths, axis=1) - all_lengths)
    group = slot_of // SLOTS
    line = offset_of[:, None] + lax.iota(jnp.int32, WINDOW)[None, :]
    usable = lax.iota(jnp.int32, WINDOW)[None, :] < length_of[:, None]
    place = group // NZ * 256 + group % NZ * HALF
    source = jnp.where(usable, place[:, None] + line // HALF * 1024 + line % HALF, 0)
    token_logprobs = jnp.where(usable, flat[source], 0.0)
    groups = jnp.sum(reward_of.reshape(SLOTS // SAMPLES, SAMPLES), axis=1)
    advantages = reward_of - (jnp.repeat(groups, SAMPLES) - reward_of) / (SAMPLES - 1.0)
    weighted = advantages * jnp.sum(token_logprobs, axis=1) / length_of.astype(F32)
    return token_logprobs, advantages, weighted


def solution(mesh):
    finer = Mesh(mesh.devices.reshape(NX, NZ, NY, NC), ("x", "z", "y", "c"))
    every = ("x", "z", "y", "c")
    placed = (P(DP, None, VOCAB), P(None, every), P(DP, None), P(DP, None), P(DP, None), P())
    return jax.shard_map(
        local, mesh=finer, in_specs=placed, out_specs=(P(DP, None), P(DP), P(DP)), check_vma=False
    )
```

```python
import jax
import jax.numpy as jnp
from jax import lax
from jax.experimental import pallas as pl
from jax.experimental.pallas import tpu as pltpu
from jax.sharding import Mesh
from jax.sharding import PartitionSpec as P

SAMPLES = 8
DP = ("x", "z")
VOCAB = ("y", "c")
REWARD_UNIT = 1.0 / 64.0
NX, NZ, NY, NC = 4, 8, 4, 2
SLOTS, WINDOW, WIDTH = 8, 14, 512
HALF = 28
MSG = 32
ROWS = NZ * HALF
META = NZ
SHARD = 501
PART = 512
TALL = ROWS + META
OFFSETS = (0, -1, 1, 2)
F32 = jnp.float32
BF16 = jnp.bfloat16
VMEM = pl.BlockSpec(memory_space=pltpu.VMEM)
SMEM = pl.BlockSpec(memory_space=pltpu.SMEM)


def params(mib=32):
    return pltpu.CompilerParams(vmem_limit_bytes=mib * 2**20)


def shift(value, axis, by):
    size = lax.axis_size(axis)
    return lax.ppermute(value, axis, [(i, (i + by) % size) for i in range(size)])


def pack_kernel(hidden_hbm, targets_hbm, lengths_hbm, rewards_hbm, out, hidden, targets, lengths, rewards, sems):
    copies = [
        pltpu.make_async_copy(src, dst, sems.at[k])
        for k, (src, dst) in enumerate(
            (
                (lengths_hbm, lengths),
                (rewards_hbm, rewards),
                (targets_hbm, targets),
                (hidden_hbm, hidden),
            )
        )
    ]
    for copy in copies:
        copy.start()
    for copy in copies:
        copy.wait()
    lane = lax.broadcasted_iota(jnp.int32, (1, 128), 1)
    offsets, both = [], jnp.zeros((1, 128), jnp.int32)
    offset_of = jnp.zeros((MSG, SLOTS), jnp.int32)
    length_of = jnp.zeros((MSG, SLOTS), jnp.int32)
    slot = lax.broadcasted_iota(jnp.int32, (MSG, SLOTS), 1)
    at = jnp.int32(0)
    for g in range(SLOTS):
        offsets.append(at)
        offset_of = jnp.where(slot == g, at, offset_of)
        length_of = jnp.where(slot == g, lengths[0, g], length_of)
        both = jnp.where(lane == g, lengths[0, g], both)
        both = jnp.where(lane == SLOTS + g, rewards[0, g], both)
        at = at + lengths[0, g]
    row_of = lax.broadcasted_iota(jnp.int32, (MSG, SLOTS), 0)
    row = lax.broadcasted_iota(jnp.int32, (MSG, WINDOW), 0)
    step = lax.broadcasted_iota(jnp.int32, (MSG, WINDOW), 1)
    wanted = targets[...]
    digits = [(wanted & 255), (wanted >> 8) & 255, wanted >> 16]
    out_row = lax.broadcasted_iota(jnp.int32, (MSG, WIDTH), 0)
    for half in range(NC):
        rows = jnp.zeros((MSG, WIDTH), F32)
        for t in range(WINDOW):
            here = (row_of + half * HALF == offset_of + t) & (t < length_of) & (row_of < HALF)
            chooser = jnp.where(here, 1.0, 0.0).astype(BF16)
            rows += jnp.dot(chooser, hidden[t], preferred_element_type=F32)
        ids = jnp.zeros((8, MSG), F32)
        for g in range(SLOTS):
            here = (row + half * HALF == offsets[g] + step) & (step < lengths[0, g]) & (row < HALF)
            chooser = jnp.where(here, 1.0, 0.0).astype(BF16)
            three = jnp.concatenate(
                [d[g : g + 1, :] for d in digits] + [jnp.zeros((5, WINDOW), jnp.int32)], axis=0
            )
            ids += lax.dot_general(
                three.astype(F32).astype(BF16),
                chooser,
                (((1,), (1,)), ((), ())),
                preferred_element_type=F32,
            )
        pad = jnp.zeros((1, 128 - MSG), F32)
        meta = jnp.concatenate(
            [ids[0:1], pad, ids[1:2], pad, ids[2:3], pad, both.astype(F32)], axis=1
        )
        message = jnp.where(out_row == HALF, meta, rows).astype(BF16)
        for z in range(NZ):
            out[z * NC + half] = message


def unpack_kernel(got, first, second):
    for core, out in enumerate((first, second)):
        pieces = [got[z * NC + core].astype(F32)[:HALF] for z in range(NZ)]
        if core == 0:
            pieces += [got[z * NC].astype(F32)[HALF : HALF + 1] for z in range(NZ)]
        out[...] = jnp.concatenate(pieces, axis=0).astype(BF16)


def join_kernel(*refs):
    out = refs[-1]
    at = 0
    for ref in refs[:-1]:
        out[at : at + ref.shape[0]] = ref[...]
        at += ref.shape[0]


def join(*parts):
    rows = sum(p.shape[0] for p in parts)
    return pl.pallas_call(
        join_kernel,
        out_shape=jax.ShapeDtypeStruct((rows, parts[0].shape[1]), BF16),
        in_specs=[VMEM] * len(parts),
        out_specs=VMEM,
        compiler_params=params(),
    )(*parts)


def gathered_line(own, axis):
    up, down, far = (shift(own, axis, by) for by in (1, -1, 2))
    return join(own, up), join(down, far)


def gathered_plane(line, axis):
    one, two = line
    up1, down1 = shift(one, axis, 1), shift(one, axis, -1)
    up2, down2 = shift(two, axis, 1), shift(two, axis, -1)
    far1, far2 = shift(up1, axis, 1), shift(down2, axis, -1)
    return (one, two), (up1, up2), (down1, down2), (far1, far2)


def stage_kernel(own, other, out):
    shard = own.shape[0]
    for k, ref in enumerate((own, other)):
        out[k * PART : k * PART + shard] = ref[...]
        out[k * PART + shard : (k + 1) * PART] = jnp.zeros((PART - shard, own.shape[1]), BF16)


def product(w, block, k):
    return lax.dot_general(
        w[:, pl.ds(pl.multiple_of(k, WIDTH), WIDTH)],
        block,
        (((1,), (1,)), ((), ())),
        preferred_element_type=F32,
    )


def matmul_kernel(which, first, last):
    def kernel(at, *refs):
        y = at[0]
        n = 2 * len(which)
        a, b, w = refs[:n], refs[n : 2 * n], refs[2 * n]
        rest = refs[2 * n + 1 :]
        if first:
            before, acc = None, rest[0]
        else:
            before, acc = rest[0], (rest[3] if last else rest[1])

        def k_of(j, core):
            return ((y + OFFSETS[j] + NY) % NY * NC + core) * WIDTH

        for i in range(NX):
            terms = []
            for p, j in enumerate(which):
                source = a[2 * p + i // 2]
                lo = i % 2 * TALL
                terms.append(product(w, source[lo : lo + ROWS, :], k_of(j, 0)))
            if i in which:
                p = which.index(i)
                for j in range(NY):
                    source = b[2 * p + j // 2]
                    lo = j % 2 * ROWS
                    terms.append(product(w, source[lo : lo + ROWS, :], k_of(j, 1)))
            total = terms[0]
            for t in terms[1:]:
                total = total + t
            if not first:
                total = total + before[i]
            acc[i] = total
        if last:
            statistics(at, rest[1], acc, rest[2], rest[4])

    return kernel


def statistics(at, ids, acc, out, held):
    x = at[1]
    held[...] = jnp.zeros_like(held)
    column = lax.broadcasted_iota(jnp.int32, (SHARD, ROWS), 0)
    for i in range(NX):
        own, other = acc[i, :SHARD], acc[i, PART : PART + SHARD]
        top = jnp.maximum(jnp.max(own, 0, keepdims=True), jnp.max(other, 0, keepdims=True))
        total = jnp.sum(jnp.exp(own - top), 0, keepdims=True) + jnp.sum(
            jnp.exp(other - top), 0, keepdims=True
        )
        wanted = ids[i : i + 1, :ROWS]
        hit = jnp.sum(jnp.where(column == wanted - at[2], own, 0.0), 0, keepdims=True)
        hit += jnp.sum(jnp.where(column == wanted - at[3], other, 0.0), 0, keepdims=True)
        x_at = (x + OFFSETS[i] + NX) % NX
        held[pl.ds(x_at, 1), :ROWS] = top + jnp.log(total)
        held[pl.ds(4 + x_at, 1), :ROWS] = hit
    for k in range(out.shape[0]):
        out[k] = held[...]


def head(at, plane0, plane1, weights, ids):
    acc_shape = jax.ShapeDtypeStruct((NX, 2 * PART, ROWS), F32)

    def call(which, before=None, last=False):
        parts = [piece for j in which for piece in plane0[j]]
        parts += [piece for j in which for piece in plane1[j]]
        inputs = [at, *parts, weights]
        first = before is None
        if not first:
            inputs.append(before)
        if last:
            inputs.append(ids)
        return pl.pallas_call(
            matmul_kernel(which, first, last),
            out_shape=jax.ShapeDtypeStruct((NX * NY, 8, 256), F32) if last else acc_shape,
            in_specs=[SMEM] + [VMEM] * (len(inputs) - 1),
            out_specs=VMEM,
            scratch_shapes=[pltpu.VMEM(acc_shape.shape, F32), pltpu.VMEM((8, 256), F32)] if last else [],
            input_output_aliases={} if first or last else {len(inputs) - 1: 0},
            compiler_params=params(14),
        )(*inputs)

    acc = call((0,))
    acc = call((1, 2), acc)
    return call((3,), acc, True)


def merged_parts(parts):
    top, hit = parts[0][:4], parts[0][4:]
    for part in parts[1:]:
        top = jnp.maximum(top, part[:4])
        hit = hit + part[4:]
    total = jnp.zeros_like(top)
    for part in parts:
        total = total + jnp.exp(part[:4] - top)
    return top + jnp.log(total), hit


def merge_kernel(parts, out):
    lse, hit = merged_parts([parts[k] for k in range(parts.shape[0])])
    for k in range(out.shape[0]):
        out[k, :4] = lse
        out[k, 4:] = hit


def final_kernel(parts, source, advantage, length, logprobs, weighted):
    tables = []
    for core in range(NC):
        lse, hit = merged_parts([parts[z * NC + core] for z in range(NZ)])
        tables.append(hit - lse)
    lane = lax.broadcasted_iota(jnp.int32, (SLOTS, 256), 1)
    wanted = source[...]
    total = jnp.zeros((SLOTS, 1), F32)
    columns = []
    for t in range(WINDOW):
        at = wanted[:, t : t + 1]
        found = jnp.zeros((SLOTS, 256), F32)
        for core in range(NC):
            for x in range(NX):
                here = at - (core * NX + x) * 256 == lane
                found = jnp.where(here, tables[core][x : x + 1, :], found)
        value = jnp.sum(found, axis=1, keepdims=True)
        columns.append(value)
        total = total + value
    logprobs[...] = jnp.concatenate(columns, axis=1)
    row = lax.broadcasted_iota(jnp.int32, (SLOTS, SLOTS), 0)
    across = lax.broadcasted_iota(jnp.int32, (SLOTS, SLOTS), 1)
    line = jnp.sum(jnp.where(row == across, total, 0.0), axis=0, keepdims=True)
    weighted[...] = advantage[...] * line / length[...]


def local(hidden, weight, targets, lengths, rewards, arrival):
    shard = weight.shape[1]
    x, z, y, c = (lax.axis_index(a) for a in ("x", "z", "y", "c"))
    swapped = shift(weight, "c", 1)
    hbm = pl.BlockSpec(memory_space=pltpu.HBM)
    sent = pl.pallas_call(
        pack_kernel,
        out_shape=jax.ShapeDtypeStruct((NZ * NC, MSG, WIDTH), BF16),
        in_specs=[hbm] * 4,
        out_specs=VMEM,
        scratch_shapes=[
            pltpu.VMEM((WINDOW, SLOTS, WIDTH), BF16),
            pltpu.VMEM((SLOTS, WINDOW), jnp.int32),
            pltpu.SMEM((1, SLOTS), jnp.int32),
            pltpu.SMEM((1, SLOTS), jnp.int32),
            pltpu.SemaphoreType.DMA((4,)),
        ],
        compiler_params=params(),
    )(hidden.transpose(1, 0, 2), targets, lengths, rewards)
    got = lax.all_to_all(sent, ("z", "c"), 0, 0, tiled=True)
    weights = pl.pallas_call(
        stage_kernel,
        out_shape=jax.ShapeDtypeStruct((2 * PART, weight.shape[0]), BF16),
        in_specs=[VMEM, VMEM],
        out_specs=VMEM,
        compiler_params=params(20),
    )(weight.T, swapped.T)
    got, weights = lax.optimization_barrier((got, weights))
    own0, own1 = pl.pallas_call(
        unpack_kernel,
        out_shape=[
            jax.ShapeDtypeStruct((TALL, WIDTH), BF16),
            jax.ShapeDtypeStruct((ROWS, WIDTH), BF16),
        ],
        in_specs=[VMEM],
        out_specs=[VMEM, VMEM],
        compiler_params=params(),
    )(got)
    line0, line1 = gathered_line(own0, "x"), gathered_line(own1, "y")
    plane0, plane1 = gathered_plane(line0, "y"), gathered_plane(line1, "x")

    metas = jnp.stack([line0[i // 2][i % 2 * TALL + ROWS : i % 2 * TALL + TALL] for i in range(NX)])
    whole = metas.astype(F32).astype(jnp.int32)
    ids = whole[:, :, :HALF] + 256 * whole[:, :, 128 : 128 + HALF] + 65536 * whole[:, :, 256 : 256 + HALF]
    ids = jnp.pad(ids.reshape(NX, ROWS), ((0, 4), (0, 0)), constant_values=-1)

    dp = x * NZ + z
    base = (dp * NY + y) * NC
    at = jnp.stack([y, x, (base + c) * shard, (base + 1 - c) * shard]).astype(jnp.int32)
    partial = head(at, plane0, plane1, weights, ids)

    order = (lax.iota(jnp.int32, NX) - x + NX) % NX
    relative = jnp.where(order == 0, 0, jnp.where(order == 3, 1, order + 1))
    per_slot = jnp.sum(
        jnp.where(
            (relative[:, None] == lax.iota(jnp.int32, NX)[None, :])[:, :, None, None],
            whole[None, :, :, 384 : 384 + 2 * SLOTS],
            0,
        ),
        axis=1,
    ).reshape(NX * NZ, 2 * SLOTS)
    all_lengths, all_rewards = per_slot[:, :SLOTS], per_slot[:, SLOTS:]
    count = NX * NZ * SLOTS
    slot_ids = lax.iota(jnp.int32, count)
    mine = lax.iota(jnp.int32, SLOTS) + dp * SLOTS
    matching = arrival[None, :] == mine[:, None]

    def lookup(table):
        return jnp.sum(jnp.where(matching, table.reshape(count)[None, :], 0), axis=1)

    slot_of = lookup(slot_ids)
    length_of = lookup(all_lengths)
    reward_of = lookup(all_rewards).astype(F32) * REWARD_UNIT
    offset_of = lookup(jnp.cumsum(all_lengths, axis=1) - all_lengths)
    group = slot_of // SLOTS
    line = offset_of[:, None] + lax.iota(jnp.int32, WINDOW)[None, :]
    usable = lax.iota(jnp.int32, WINDOW)[None, :] < length_of[:, None]
    place = group // NZ * 256 + group % NZ * HALF
    source = jnp.where(usable, place[:, None] + line // HALF * 1024 + line % HALF, -1)
    groups = jnp.sum(reward_of.reshape(SLOTS // SAMPLES, SAMPLES), axis=1)
    advantages = reward_of - (jnp.repeat(groups, SAMPLES) - reward_of) / (SAMPLES - 1.0)

    stats = lax.all_to_all(partial, ("x", "y"), 0, 0, tiled=True)
    stats = pl.pallas_call(
        merge_kernel,
        out_shape=jax.ShapeDtypeStruct((NZ * NC, 8, 256), F32),
        in_specs=[VMEM],
        out_specs=VMEM,
        compiler_params=params(),
    )(stats)
    stats = lax.all_to_all(stats, ("z", "c"), 0, 0, tiled=True)
    token_logprobs, weighted = pl.pallas_call(
        final_kernel,
        out_shape=[
            jax.ShapeDtypeStruct((SLOTS, WINDOW), F32),
            jax.ShapeDtypeStruct((1, SLOTS), F32),
        ],
        in_specs=[VMEM] * 4,
        out_specs=[VMEM, VMEM],
        compiler_params=params(),
    )(stats, source, advantages[None, :], length_of.astype(F32)[None, :])
    return token_logprobs, advantages, weighted.reshape(SLOTS)


def solution(mesh):
    finer = Mesh(mesh.devices.reshape(NX, NZ, NY, NC), ("x", "z", "y", "c"))
    every = ("x", "z", "y", "c")
    placed = (P(DP, None, VOCAB), P(None, every), P(DP, None), P(DP, None), P(DP, None), P())
    return jax.shard_map(
        local, mesh=finer, in_specs=placed, out_specs=(P(DP, None), P(DP), P(DP)), check_vma=False
    )
```

```python
import jax
import jax.numpy as jnp
from jax import lax
from jax.experimental import pallas as pl
from jax.experimental.pallas import tpu as pltpu
from jax.sharding import Mesh
from jax.sharding import PartitionSpec as P


SAMPLES = 8
DP = ("x", "z")
VOCAB = ("y", "c")
REWARD_UNIT = 1.0 / 64.0
NX, NZ, NY, NC = 4, 8, 4, 2
SLOTS, WINDOW, WIDTH = 8, 14, 512
HALF = 28
MSG = 32
ROWS = NZ * HALF
META = NZ
SHARD = 501
TALL = ROWS + META
OFFSETS = (0, -1, 1, 2)
F32 = jnp.float32
BF16 = jnp.bfloat16
VMEM = pl.BlockSpec(memory_space=pltpu.VMEM)
SMEM = pl.BlockSpec(memory_space=pltpu.SMEM)
HBM = pl.BlockSpec(memory_space=pltpu.HBM)


def params(mib=32):
    return pltpu.CompilerParams(vmem_limit_bytes=mib * 2**20)


def in_hbm(*arrays):
    return [pltpu.with_memory_space_constraint(a, pltpu.HBM) for a in arrays]


def shift(value, axis, by):
    size = lax.axis_size(axis)
    return lax.ppermute(value, axis, [(i, (i + by) % size) for i in range(size)])


def pack_kernel(hidden_hbm, targets_hbm, lengths_hbm, rewards_hbm, out, hidden, targets, lengths, rewards, sems):
    copies = [
        pltpu.make_async_copy(src, dst, sems.at[k])
        for k, (src, dst) in enumerate(
            (
                (lengths_hbm, lengths),
                (rewards_hbm, rewards),
                (targets_hbm, targets),
                (hidden_hbm, hidden),
            )
        )
    ]
    for copy in copies:
        copy.start()
    for copy in copies:
        copy.wait()
    lane = lax.broadcasted_iota(jnp.int32, (1, 128), 1)
    offsets, both = [], jnp.zeros((1, 128), jnp.int32)
    offset_of = jnp.zeros((MSG, SLOTS), jnp.int32)
    length_of = jnp.zeros((MSG, SLOTS), jnp.int32)
    slot = lax.broadcasted_iota(jnp.int32, (MSG, SLOTS), 1)
    at = jnp.int32(0)
    for g in range(SLOTS):
        offsets.append(at)
        offset_of = jnp.where(slot == g, at, offset_of)
        length_of = jnp.where(slot == g, lengths[0, g], length_of)
        both = jnp.where(lane == g, lengths[0, g], both)
        both = jnp.where(lane == SLOTS + g, rewards[0, g], both)
        at = at + lengths[0, g]
    row_of = lax.broadcasted_iota(jnp.int32, (MSG, SLOTS), 0)
    row = lax.broadcasted_iota(jnp.int32, (MSG, WINDOW), 0)
    step = lax.broadcasted_iota(jnp.int32, (MSG, WINDOW), 1)
    wanted = targets[...]
    digits = [(wanted & 255), (wanted >> 8) & 255, wanted >> 16]
    out_row = lax.broadcasted_iota(jnp.int32, (MSG, WIDTH), 0)
    for half in range(NC):
        rows = jnp.zeros((MSG, WIDTH), F32)
        for t in range(WINDOW):
            here = (row_of + half * HALF == offset_of + t) & (t < length_of) & (row_of < HALF)
            chooser = jnp.where(here, 1.0, 0.0).astype(BF16)
            rows += jnp.dot(chooser, hidden[t], preferred_element_type=F32)
        ids = jnp.zeros((8, MSG), F32)
        for g in range(SLOTS):
            here = (row + half * HALF == offsets[g] + step) & (step < lengths[0, g]) & (row < HALF)
            chooser = jnp.where(here, 1.0, 0.0).astype(BF16)
            three = jnp.concatenate(
                [d[g : g + 1, :] for d in digits] + [jnp.zeros((5, WINDOW), jnp.int32)], axis=0
            )
            ids += lax.dot_general(
                three.astype(F32).astype(BF16),
                chooser,
                (((1,), (1,)), ((), ())),
                preferred_element_type=F32,
            )
        pad = jnp.zeros((1, 128 - MSG), F32)
        meta = jnp.concatenate(
            [ids[0:1], pad, ids[1:2], pad, ids[2:3], pad, both.astype(F32)], axis=1
        )
        message = jnp.where(out_row == HALF, meta, rows).astype(BF16)
        for z in range(NZ):
            out[z * NC + half] = message


def unpack_kernel(got, first, second):
    for core, out in enumerate((first, second)):
        pieces = [got[z * NC + core].astype(F32)[:HALF] for z in range(NZ)]
        if core == 0:
            pieces += [got[z * NC].astype(F32)[HALF : HALF + 1] for z in range(NZ)]
        out[...] = jnp.concatenate(pieces, axis=0).astype(BF16)


def join_kernel(one, two, out):
    out[: one.shape[0]] = one[...]
    out[one.shape[0] :] = two[...]


def join(one, two):
    return pl.pallas_call(
        join_kernel,
        out_shape=jax.ShapeDtypeStruct((one.shape[0] + two.shape[0], one.shape[1]), BF16),
        in_specs=[VMEM, VMEM],
        out_specs=VMEM,
        compiler_params=params(),
    )(one, two)


def gathered_planes(own, firsts, lasts):
    both = range(2)
    up = [shift(own[k], firsts[k], 1) for k in both]
    down = [shift(own[k], firsts[k], -1) for k in both]
    far = [shift(up[k], firsts[k], 1) for k in both]
    one = [join(own[k], up[k]) for k in both]
    two = [join(down[k], far[k]) for k in both]
    planes = []
    for k in both:
        up1 = shift(one[k], lasts[k], 1)
        down1 = shift(one[k], lasts[k], -1)
        down2 = shift(two[k], lasts[k], -1)
        up2 = shift(two[k], lasts[k], 1)
        far2 = shift(down2, lasts[k], -1)
        far1 = shift(up1, lasts[k], 1)
        planes.append(((one[k], two[k]), (up1, up2), (down1, down2), (far1, far2)))
    return planes


def product(w, block):
    return lax.dot_general(w[...], block, (((1,), (1,)), ((), ())), preferred_element_type=F32)


def matmul_kernel(which, last):
    def kernel(at, *refs):
        y = at[0]
        n = 2 * len(which)
        a, b, weights, rest = refs[:n], refs[n : 2 * n], refs[2 * n : 2 * n + 2], refs[2 * n + 2 :]
        if last:
            before, ids, out, acc, held, held_w, sems = rest
        else:
            acc, held_w, sems = rest
        wanted = [(j, 0) for j in which] + [(j, 1) for j in range(NY)]
        copies = {}
        for k, (j, core) in enumerate(wanted):
            column = pl.multiple_of(((y + OFFSETS[j] + NY) % NY * NC + core) * WIDTH, WIDTH)
            copies[j, core] = [
                pltpu.make_async_copy(
                    weights[w].at[:, pl.ds(column, WIDTH)], held_w.at[k, w], sems.at[k, w]
                )
                for w in range(2)
            ]
            for copy in copies[j, core]:
                copy.start()
        ready = set()
        for i in [i for i in range(NX) if i not in which] + list(which):
            terms = []
            for p, j in enumerate(which):
                lo = i % 2 * TALL
                terms.append(((j, 0), a[2 * p + i // 2][lo : lo + ROWS, :]))
            if i in which:
                p = which.index(i)
                for j in range(NY):
                    lo = j % 2 * ROWS
                    terms.append(((j, 1), b[2 * p + j // 2][lo : lo + ROWS, :]))
            for key, _ in terms:
                if key not in ready:
                    ready.add(key)
                    for copy in copies[key]:
                        copy.wait()
            for w in range(2):
                total = before[i, w] if last else None
                for key, block in terms:
                    term = product(held_w.at[wanted.index(key), w], block)
                    total = term if total is None else total + term
                acc[i, w] = total
        if last:
            statistics(at, ids, acc, out, held)

    return kernel


def statistics(at, ids, acc, out, held):
    x = at[1]
    held[...] = jnp.zeros_like(held)
    column = lax.broadcasted_iota(jnp.int32, (SHARD, ROWS), 0)
    for i in range(NX):
        own, other = acc[i, 0], acc[i, 1]
        top = jnp.maximum(jnp.max(own, 0, keepdims=True), jnp.max(other, 0, keepdims=True))
        total = jnp.sum(jnp.exp(own - top), 0, keepdims=True) + jnp.sum(
            jnp.exp(other - top), 0, keepdims=True
        )
        wanted = ids[i : i + 1, :ROWS]
        hit = jnp.sum(jnp.where(column == wanted - at[2], own, 0.0), 0, keepdims=True)
        hit += jnp.sum(jnp.where(column == wanted - at[3], other, 0.0), 0, keepdims=True)
        x_at = (x + OFFSETS[i] + NX) % NX
        held[pl.ds(x_at, 1), :ROWS] = top + jnp.log(total)
        held[pl.ds(4 + x_at, 1), :ROWS] = hit
    for k in range(out.shape[0]):
        out[k] = held[...]


def head(at, plane0, plane1, weights, ids):
    acc_shape = (NX, 2, SHARD, ROWS)

    def call(which, *more):
        parts = [piece for j in which for piece in plane0[j]]
        parts += [piece for j in which for piece in plane1[j]]
        last = bool(more)
        slices = len(which) + NY
        scratch = [pltpu.VMEM(acc_shape, F32), pltpu.VMEM((8, 256), F32)] if last else []
        scratch += [
            pltpu.VMEM((slices, 2, SHARD, WIDTH), BF16),
            pltpu.SemaphoreType.DMA((slices, 2)),
        ]
        shape = (NX * NY, 8, 256) if last else acc_shape
        return pl.pallas_call(
            matmul_kernel(which, last),
            out_shape=jax.ShapeDtypeStruct(shape, F32),
            in_specs=[SMEM] + [VMEM] * len(parts) + [HBM] * 2 + [VMEM] * len(more),
            out_specs=VMEM,
            scratch_shapes=scratch,
            compiler_params=params(26),
        )(at, *parts, *weights, *more)

    acc = call((0, 1, 2))
    return call((3,), acc, ids)


def merged_parts(parts):
    top, hit = parts[0][:4], parts[0][4:]
    for part in parts[1:]:
        top = jnp.maximum(top, part[:4])
        hit = hit + part[4:]
    total = jnp.zeros_like(top)
    for part in parts:
        total = total + jnp.exp(part[:4] - top)
    return top + jnp.log(total), hit


def merge_kernel(parts, out):
    lse, hit = merged_parts([parts[k] for k in range(parts.shape[0])])
    for k in range(out.shape[0]):
        out[k, :4] = lse
        out[k, 4:] = hit


def final_kernel(parts, source, advantage, length, logprobs, weighted):
    tables = []
    for core in range(NC):
        lse, hit = merged_parts([parts[z * NC + core] for z in range(NZ)])
        tables.append(hit - lse)
    lane = lax.broadcasted_iota(jnp.int32, (SLOTS, 256), 1)
    wanted = source[...]
    total = jnp.zeros((SLOTS, 1), F32)
    columns = []
    for t in range(WINDOW):
        at = wanted[:, t : t + 1]
        found = jnp.zeros((SLOTS, 256), F32)
        for core in range(NC):
            for x in range(NX):
                here = at - (core * NX + x) * 256 == lane
                found = jnp.where(here, tables[core][x : x + 1, :], found)
        value = jnp.sum(found, axis=1, keepdims=True)
        columns.append(value)
        total = total + value
    logprobs[...] = jnp.concatenate(columns, axis=1)
    row = lax.broadcasted_iota(jnp.int32, (SLOTS, SLOTS), 0)
    across = lax.broadcasted_iota(jnp.int32, (SLOTS, SLOTS), 1)
    line = jnp.sum(jnp.where(row == across, total, 0.0), axis=0, keepdims=True)
    weighted[...] = advantage[...] * line / length[...]


def local(hidden, weight, targets, lengths, rewards, arrival):
    shard = weight.shape[1]
    x, z, y, c = (lax.axis_index(a) for a in ("x", "z", "y", "c"))
    swapped = shift(weight, "c", 1)
    sent = pl.pallas_call(
        pack_kernel,
        out_shape=jax.ShapeDtypeStruct((NZ * NC, MSG, WIDTH), BF16),
        in_specs=[HBM] * 4,
        out_specs=VMEM,
        scratch_shapes=[
            pltpu.VMEM((WINDOW, SLOTS, WIDTH), BF16),
            pltpu.VMEM((SLOTS, WINDOW), jnp.int32),
            pltpu.SMEM((1, SLOTS), jnp.int32),
            pltpu.SMEM((1, SLOTS), jnp.int32),
            pltpu.SemaphoreType.DMA((4,)),
        ],
        compiler_params=params(),
    )(*in_hbm(hidden.transpose(1, 0, 2), targets, lengths, rewards))
    got = lax.all_to_all(sent, ("z", "c"), 0, 0, tiled=True)
    own0, own1 = pl.pallas_call(
        unpack_kernel,
        out_shape=[
            jax.ShapeDtypeStruct((TALL, WIDTH), BF16),
            jax.ShapeDtypeStruct((ROWS, WIDTH), BF16),
        ],
        in_specs=[VMEM],
        out_specs=[VMEM, VMEM],
        compiler_params=params(),
    )(got)
    plane0, plane1 = gathered_planes((own0, own1), ("x", "y"), ("y", "x"))
    line0 = plane0[0]

    metas = jnp.stack([line0[i // 2][i % 2 * TALL + ROWS : i % 2 * TALL + TALL] for i in range(NX)])
    whole = metas.astype(F32).astype(jnp.int32)
    ids = whole[:, :, :HALF] + 256 * whole[:, :, 128 : 128 + HALF] + 65536 * whole[:, :, 256 : 256 + HALF]
    ids = jnp.pad(ids.reshape(NX, ROWS), ((0, 4), (0, 0)), constant_values=-1)

    dp = x * NZ + z
    base = (dp * NY + y) * NC
    at = jnp.stack([y, x, (base + c) * shard, (base + 1 - c) * shard]).astype(jnp.int32)
    partial = head(at, plane0, plane1, in_hbm(weight.T, swapped.T), ids)

    order = (lax.iota(jnp.int32, NX) - x + NX) % NX
    relative = jnp.where(order == 0, 0, jnp.where(order == 3, 1, order + 1))
    per_slot = jnp.sum(
        jnp.where(
            (relative[:, None] == lax.iota(jnp.int32, NX)[None, :])[:, :, None, None],
            whole[None, :, :, 384 : 384 + 2 * SLOTS],
            0,
        ),
        axis=1,
    ).reshape(NX * NZ, 2 * SLOTS)
    all_lengths, all_rewards = per_slot[:, :SLOTS], per_slot[:, SLOTS:]
    count = NX * NZ * SLOTS
    slot_ids = lax.iota(jnp.int32, count)
    mine = lax.iota(jnp.int32, SLOTS) + dp * SLOTS
    matching = arrival[None, :] == mine[:, None]

    def lookup(table):
        return jnp.sum(jnp.where(matching, table.reshape(count)[None, :], 0), axis=1)

    slot_of = lookup(slot_ids)
    length_of = lookup(all_lengths)
    reward_of = lookup(all_rewards).astype(F32) * REWARD_UNIT
    offset_of = lookup(jnp.cumsum(all_lengths, axis=1) - all_lengths)
    group = slot_of // SLOTS
    line = offset_of[:, None] + lax.iota(jnp.int32, WINDOW)[None, :]
    usable = lax.iota(jnp.int32, WINDOW)[None, :] < length_of[:, None]
    place = group // NZ * 256 + group % NZ * HALF
    source = jnp.where(usable, place[:, None] + line // HALF * 1024 + line % HALF, -1)
    groups = jnp.sum(reward_of.reshape(SLOTS // SAMPLES, SAMPLES), axis=1)
    advantages = reward_of - (jnp.repeat(groups, SAMPLES) - reward_of) / (SAMPLES - 1.0)

    stats = lax.all_to_all(partial, ("x", "y"), 0, 0, tiled=True)
    stats = pl.pallas_call(
        merge_kernel,
        out_shape=jax.ShapeDtypeStruct((NZ * NC, 8, 256), F32),
        in_specs=[VMEM],
        out_specs=VMEM,
        compiler_params=params(),
    )(stats)
    stats = lax.all_to_all(stats, ("z", "c"), 0, 0, tiled=True)
    token_logprobs, weighted = pl.pallas_call(
        final_kernel,
        out_shape=[
            jax.ShapeDtypeStruct((SLOTS, WINDOW), F32),
            jax.ShapeDtypeStruct((1, SLOTS), F32),
        ],
        in_specs=[VMEM] * 4,
        out_specs=[VMEM, VMEM],
        compiler_params=params(),
    )(stats, source, advantages[None, :], length_of.astype(F32)[None, :])
    return token_logprobs, advantages, weighted.reshape(SLOTS)


def solution(mesh):
    finer = Mesh(mesh.devices.reshape(NX, NZ, NY, NC), ("x", "z", "y", "c"))
    every = ("x", "z", "y", "c")
    placed = (P(DP, None, VOCAB), P(None, every), P(DP, None), P(DP, None), P(DP, None), P())

    return jax.shard_map(
        local, mesh=finer, in_specs=placed, out_specs=(P(DP, None), P(DP), P(DP)), check_vma=False
    )
```

```python
import jax
import jax.numpy as jnp
from jax import lax
from jax.experimental import pallas as pl
from jax.experimental.pallas import tpu as pltpu
from jax.sharding import Mesh
from jax.sharding import PartitionSpec as P


SAMPLES = 8
DP = ("x", "z")
VOCAB = ("y", "c")
REWARD_UNIT = 1.0 / 64.0
NX, NZ, NY, NC = 4, 8, 4, 2
SLOTS, WINDOW, WIDTH = 8, 14, 512
HALF = 28
MSG = 32
ROWS = NZ * HALF
META = NZ
SHARD = 501
TALL = ROWS + META
OFFSETS = (0, -1, 1, 2)
F32 = jnp.float32
BF16 = jnp.bfloat16
VMEM = pl.BlockSpec(memory_space=pltpu.VMEM)
SMEM = pl.BlockSpec(memory_space=pltpu.SMEM)
HBM = pl.BlockSpec(memory_space=pltpu.HBM)


def params(mib=32):
    return pltpu.CompilerParams(vmem_limit_bytes=mib * 2**20)


def in_hbm(*arrays):
    return [pltpu.with_memory_space_constraint(a, pltpu.HBM) for a in arrays]


def shift(value, axis, by):
    size = lax.axis_size(axis)
    return lax.ppermute(value, axis, [(i, (i + by) % size) for i in range(size)])


def pack_kernel(hidden_hbm, targets_hbm, lengths_hbm, rewards_hbm, out, hidden, targets, lengths, rewards, sems):
    copies = [
        pltpu.make_async_copy(src, dst, sems.at[k])
        for k, (src, dst) in enumerate(
            (
                (lengths_hbm, lengths),
                (rewards_hbm, rewards),
                (targets_hbm, targets),
                (hidden_hbm, hidden),
            )
        )
    ]
    for copy in copies:
        copy.start()
    for copy in copies:
        copy.wait()
    lane = lax.broadcasted_iota(jnp.int32, (1, 128), 1)
    offsets, both = [], jnp.zeros((1, 128), jnp.int32)
    offset_of = jnp.zeros((MSG, SLOTS), jnp.int32)
    length_of = jnp.zeros((MSG, SLOTS), jnp.int32)
    slot = lax.broadcasted_iota(jnp.int32, (MSG, SLOTS), 1)
    at = jnp.int32(0)
    for g in range(SLOTS):
        offsets.append(at)
        offset_of = jnp.where(slot == g, at, offset_of)
        length_of = jnp.where(slot == g, lengths[0, g], length_of)
        both = jnp.where(lane == g, lengths[0, g], both)
        both = jnp.where(lane == SLOTS + g, rewards[0, g], both)
        at = at + lengths[0, g]
    row_of = lax.broadcasted_iota(jnp.int32, (MSG, SLOTS), 0)
    row = lax.broadcasted_iota(jnp.int32, (MSG, WINDOW), 0)
    step = lax.broadcasted_iota(jnp.int32, (MSG, WINDOW), 1)
    wanted = targets[...]
    digits = [(wanted & 255), (wanted >> 8) & 255, wanted >> 16]
    out_row = lax.broadcasted_iota(jnp.int32, (MSG, WIDTH), 0)
    for half in range(NC):
        rows = jnp.zeros((MSG, WIDTH), F32)
        for t in range(WINDOW):
            here = (row_of + half * HALF == offset_of + t) & (t < length_of) & (row_of < HALF)
            chooser = jnp.where(here, 1.0, 0.0).astype(BF16)
            rows += jnp.dot(chooser, hidden[t], preferred_element_type=F32)
        ids = jnp.zeros((8, MSG), F32)
        for g in range(SLOTS):
            here = (row + half * HALF == offsets[g] + step) & (step < lengths[0, g]) & (row < HALF)
            chooser = jnp.where(here, 1.0, 0.0).astype(BF16)
            three = jnp.concatenate(
                [d[g : g + 1, :] for d in digits] + [jnp.zeros((5, WINDOW), jnp.int32)], axis=0
            )
            ids += lax.dot_general(
                three.astype(F32).astype(BF16),
                chooser,
                (((1,), (1,)), ((), ())),
                preferred_element_type=F32,
            )
        pad = jnp.zeros((1, 128 - MSG), F32)
        meta = jnp.concatenate(
            [ids[0:1], pad, ids[1:2], pad, ids[2:3], pad, both.astype(F32)], axis=1
        )
        message = jnp.where(out_row == HALF, meta, rows).astype(BF16)
        for z in range(NZ):
            out[z * NC + half] = message


def unpack_kernel(got, first, second):
    for core, out in enumerate((first, second)):
        pieces = [got[z * NC + core].astype(F32)[:HALF] for z in range(NZ)]
        if core == 0:
            pieces += [got[z * NC].astype(F32)[HALF : HALF + 1] for z in range(NZ)]
        out[...] = jnp.concatenate(pieces, axis=0).astype(BF16)


def join_kernel(one, two, out):
    out[: one.shape[0]] = one[...]
    out[one.shape[0] :] = two[...]


def join(one, two):
    return pl.pallas_call(
        join_kernel,
        out_shape=jax.ShapeDtypeStruct((one.shape[0] + two.shape[0], one.shape[1]), BF16),
        in_specs=[VMEM, VMEM],
        out_specs=VMEM,
        compiler_params=params(),
    )(one, two)


def gathered_planes(own, firsts, lasts):
    both = range(2)
    up = [shift(own[k], firsts[k], 1) for k in both]
    down = [shift(own[k], firsts[k], -1) for k in both]
    far = [shift(up[k], firsts[k], 1) for k in both]
    one = [join(own[k], up[k]) for k in both]
    two = [join(down[k], far[k]) for k in both]
    planes = []
    for k in both:
        up1 = shift(one[k], lasts[k], 1)
        down1 = shift(one[k], lasts[k], -1)
        down2 = shift(two[k], lasts[k], -1)
        up2 = shift(two[k], lasts[k], 1)
        far2 = shift(down2, lasts[k], -1)
        far1 = shift(up1, lasts[k], 1)
        planes.append(((one[k], two[k]), (up1, up2), (down1, down2), (far1, far2)))
    return planes


def product(w, block):
    return lax.dot_general(w[...], block, (((1,), (1,)), ((), ())), preferred_element_type=F32)


def matmul_kernel(which, on_chip, first, last):
    names = [(k, j, part) for k in range(2) for j in which for part in range(2)]

    def kernel(at, *refs):
        y = at[0]
        pieces = dict(zip(names, refs))
        refs = refs[len(names) :]
        weights, refs = refs[:2], refs[2:]
        before = None
        if not first:
            before, refs = refs[0], refs[1:]
        if last:
            ids, out, acc, held, held_p, held_w, sems, sems_w, sems_a = refs
        else:
            out, acc, held_p, held_w, sems, sems_w, sems_a = refs

        plan = []
        for i in [i for i in range(NX) if i not in which] + list(which):
            terms = []
            for j in which:
                terms.append(((j, 0), (0, j, i // 2), i % 2 * TALL))
            if i in which:
                terms += [((j, 1), (1, i, j // 2), j % 2 * ROWS) for j in range(NY)]
            plan.append((i, terms))

        slices, moved, waits, views = {}, {}, {}, {}
        for i, terms in plan:
            if not first:
                waits[i] = [pltpu.make_async_copy(before.at[i], acc.at[i], sems_a.at[i])]
                waits[i][0].start()
            for key, name, _ in terms:
                if key not in slices:
                    n = slices[key] = len(slices)
                    j, colour = key
                    row = (y + OFFSETS[j] + NY) % NY * NC
                    column = pl.multiple_of((row + colour) * WIDTH, WIDTH)
                    waits[key] = [
                        pltpu.make_async_copy(
                            weights[w].at[:, pl.ds(column, WIDTH)], held_w.at[n, w], sems_w.at[n, w]
                        )
                        for w in range(2)
                    ]
                    for copy in waits[key]:
                        copy.start()
                if name not in views:
                    ref = pieces[name]
                    if on_chip(name):
                        views[name] = ref
                    else:
                        n = moved[name] = len(moved)
                        views[name] = held_p.at[n]
                        copy = pltpu.make_async_copy(
                            ref, held_p.at[n, pl.ds(0, ref.shape[0])], sems.at[n]
                        )
                        copy.start()
                        waits[name] = [copy]

        def ready(key):
            for copy in waits.pop(key, ()):
                copy.wait()

        leaving = []
        for i, terms in plan:
            ready(i)
            for key, name, _ in terms:
                ready(key)
                ready(name)
            for w in range(2):
                total = None if first else acc[i, w]
                for key, name, lo in terms:
                    term = product(held_w.at[slices[key], w], views[name][lo : lo + ROWS, :])
                    total = term if total is None else total + term
                acc[i, w] = total
            if not last:
                leaving.append(pltpu.make_async_copy(acc.at[i], out.at[i], sems_a.at[i]))
                leaving[-1].start()
        if last:
            statistics(at, ids, acc, out, held)
        for copy in leaving:
            copy.wait()

    return kernel


def statistics(at, ids, acc, out, held):
    x = at[1]
    held[...] = jnp.zeros_like(held)
    column = lax.broadcasted_iota(jnp.int32, (SHARD, ROWS), 0)
    for i in range(NX):
        own, other = acc[i, 0], acc[i, 1]
        top = jnp.maximum(jnp.max(own, 0, keepdims=True), jnp.max(other, 0, keepdims=True))
        total = jnp.sum(jnp.exp(own - top), 0, keepdims=True) + jnp.sum(
            jnp.exp(other - top), 0, keepdims=True
        )
        wanted = ids[i : i + 1, :ROWS]
        hit = jnp.sum(jnp.where(column == wanted - at[2], own, 0.0), 0, keepdims=True)
        hit += jnp.sum(jnp.where(column == wanted - at[3], other, 0.0), 0, keepdims=True)
        x_at = (x + OFFSETS[i] + NX) % NX
        held[pl.ds(x_at, 1), :ROWS] = top + jnp.log(total)
        held[pl.ds(4 + x_at, 1), :ROWS] = hit
    for k in range(out.shape[0]):
        out[k] = held[...]


def head(at, planes, weights, ids):
    acc_shape = (NX, 2, SHARD, ROWS)

    def call(which, on_chip, first, last, *more):
        names = [(k, j, part) for k in range(2) for j in which for part in range(2)]
        parts, specs = [], []
        for name in names:
            piece = planes[name[0]][name[1]][name[2]]
            parts += [piece] if on_chip(name) else in_hbm(piece)
            specs.append(VMEM if on_chip(name) else HBM)
        slices = len(which) + NY
        late = max(1, sum(not on_chip(name) for name in names))
        scratch = [pltpu.VMEM(acc_shape, F32)] + ([pltpu.VMEM((8, 256), F32)] if last else [])
        scratch += [
            pltpu.VMEM((late, 2 * TALL, WIDTH), BF16),
            pltpu.VMEM((slices, 2, SHARD, WIDTH), BF16),
            pltpu.SemaphoreType.DMA((late,)),
            pltpu.SemaphoreType.DMA((slices, 2)),
            pltpu.SemaphoreType.DMA((NX,)),
        ]
        shape = (NX * NY, 8, 256) if last else acc_shape
        specs = [SMEM] + specs + [HBM] * 2
        specs += [] if first else [HBM]
        specs += [VMEM] if last else []
        return pl.pallas_call(
            matmul_kernel(which, on_chip, first, last),
            out_shape=pltpu.VMEM(shape, F32) if last else pltpu.HBM(shape, F32),
            in_specs=specs,
            out_specs=VMEM if last else HBM,
            scratch_shapes=scratch,
            compiler_params=params(24),
        )(at, *parts, *weights, *more)

    (acc,) = in_hbm(call((0,), lambda name: True, True, False))
    (acc,) = in_hbm(call((1, 2), lambda name: name[1] - 1 == name[2], False, False, acc))
    return call((3,), lambda name: False, False, True, acc, ids)


def merged_parts(parts):
    top, hit = parts[0][:4], parts[0][4:]
    for part in parts[1:]:
        top = jnp.maximum(top, part[:4])
        hit = hit + part[4:]
    total = jnp.zeros_like(top)
    for part in parts:
        total = total + jnp.exp(part[:4] - top)
    return top + jnp.log(total), hit


def merge_kernel(parts, out):
    lse, hit = merged_parts([parts[k] for k in range(parts.shape[0])])
    for k in range(out.shape[0]):
        out[k, :4] = lse
        out[k, 4:] = hit


def final_kernel(parts, source, advantage, length, logprobs, weighted):
    tables = []
    for core in range(NC):
        lse, hit = merged_parts([parts[z * NC + core] for z in range(NZ)])
        tables.append(hit - lse)
    lane = lax.broadcasted_iota(jnp.int32, (SLOTS, 256), 1)
    wanted = source[...]
    total = jnp.zeros((SLOTS, 1), F32)
    columns = []
    for t in range(WINDOW):
        at = wanted[:, t : t + 1]
        found = jnp.zeros((SLOTS, 256), F32)
        for core in range(NC):
            for x in range(NX):
                here = at - (core * NX + x) * 256 == lane
                found = jnp.where(here, tables[core][x : x + 1, :], found)
        value = jnp.sum(found, axis=1, keepdims=True)
        columns.append(value)
        total = total + value
    logprobs[...] = jnp.concatenate(columns, axis=1)
    row = lax.broadcasted_iota(jnp.int32, (SLOTS, SLOTS), 0)
    across = lax.broadcasted_iota(jnp.int32, (SLOTS, SLOTS), 1)
    line = jnp.sum(jnp.where(row == across, total, 0.0), axis=0, keepdims=True)
    weighted[...] = advantage[...] * line / length[...]


def local(hidden, weight, targets, lengths, rewards, arrival):
    shard = weight.shape[1]
    x, z, y, c = (lax.axis_index(a) for a in ("x", "z", "y", "c"))
    swapped = shift(weight, "c", 1)
    sent = pl.pallas_call(
        pack_kernel,
        out_shape=pltpu.VMEM((NZ * NC, MSG, WIDTH), BF16),
        in_specs=[HBM] * 4,
        out_specs=VMEM,
        scratch_shapes=[
            pltpu.VMEM((WINDOW, SLOTS, WIDTH), BF16),
            pltpu.VMEM((SLOTS, WINDOW), jnp.int32),
            pltpu.SMEM((1, SLOTS), jnp.int32),
            pltpu.SMEM((1, SLOTS), jnp.int32),
            pltpu.SemaphoreType.DMA((4,)),
        ],
        compiler_params=params(),
    )(*in_hbm(hidden.transpose(1, 0, 2), targets, lengths, rewards))
    got = lax.all_to_all(sent, ("z", "c"), 0, 0, tiled=True)
    own0, own1 = pl.pallas_call(
        unpack_kernel,
        out_shape=[
            jax.ShapeDtypeStruct((TALL, WIDTH), BF16),
            jax.ShapeDtypeStruct((ROWS, WIDTH), BF16),
        ],
        in_specs=[VMEM],
        out_specs=[VMEM, VMEM],
        compiler_params=params(),
    )(got)
    planes = gathered_planes((own0, own1), ("x", "y"), ("y", "x"))
    line0 = planes[0][0]

    metas = jnp.stack([line0[i // 2][i % 2 * TALL + ROWS : i % 2 * TALL + TALL] for i in range(NX)])
    whole = metas.astype(F32).astype(jnp.int32)
    ids = whole[:, :, :HALF] + 256 * whole[:, :, 128 : 128 + HALF] + 65536 * whole[:, :, 256 : 256 + HALF]
    ids = jnp.pad(ids.reshape(NX, ROWS), ((0, 4), (0, 0)), constant_values=-1)

    dp = x * NZ + z
    base = (dp * NY + y) * NC
    at = jnp.stack([y, x, (base + c) * shard, (base + 1 - c) * shard]).astype(jnp.int32)
    partial = head(at, planes, in_hbm(weight.T, swapped.T), ids)

    order = (lax.iota(jnp.int32, NX) - x + NX) % NX
    relative = jnp.where(order == 0, 0, jnp.where(order == 3, 1, order + 1))
    per_slot = jnp.sum(
        jnp.where(
            (relative[:, None] == lax.iota(jnp.int32, NX)[None, :])[:, :, None, None],
            whole[None, :, :, 384 : 384 + 2 * SLOTS],
            0,
        ),
        axis=1,
    ).reshape(NX * NZ, 2 * SLOTS)
    all_lengths, all_rewards = per_slot[:, :SLOTS], per_slot[:, SLOTS:]
    count = NX * NZ * SLOTS
    slot_ids = lax.iota(jnp.int32, count)
    mine = lax.iota(jnp.int32, SLOTS) + dp * SLOTS
    matching = arrival[None, :] == mine[:, None]

    def lookup(table):
        return jnp.sum(jnp.where(matching, table.reshape(count)[None, :], 0), axis=1)

    slot_of = lookup(slot_ids)
    length_of = lookup(all_lengths)
    reward_of = lookup(all_rewards).astype(F32) * REWARD_UNIT
    offset_of = lookup(jnp.cumsum(all_lengths, axis=1) - all_lengths)
    group = slot_of // SLOTS
    line = offset_of[:, None] + lax.iota(jnp.int32, WINDOW)[None, :]
    usable = lax.iota(jnp.int32, WINDOW)[None, :] < length_of[:, None]
    place = group // NZ * 256 + group % NZ * HALF
    source = jnp.where(usable, place[:, None] + line // HALF * 1024 + line % HALF, -1)
    groups = jnp.sum(reward_of.reshape(SLOTS // SAMPLES, SAMPLES), axis=1)
    advantages = reward_of - (jnp.repeat(groups, SAMPLES) - reward_of) / (SAMPLES - 1.0)

    stats = lax.all_to_all(partial, ("x", "y"), 0, 0, tiled=True)
    stats = pl.pallas_call(
        merge_kernel,
        out_shape=pltpu.VMEM((NZ * NC, 8, 256), F32),
        in_specs=[VMEM],
        out_specs=VMEM,
        compiler_params=params(),
    )(stats)
    stats = lax.all_to_all(stats, ("z", "c"), 0, 0, tiled=True)
    token_logprobs, weighted = pl.pallas_call(
        final_kernel,
        out_shape=[
            jax.ShapeDtypeStruct((SLOTS, WINDOW), F32),
            jax.ShapeDtypeStruct((1, SLOTS), F32),
        ],
        in_specs=[VMEM] * 4,
        out_specs=[VMEM, VMEM],
        compiler_params=params(),
    )(stats, source, advantages[None, :], length_of.astype(F32)[None, :])
    return token_logprobs, advantages, weighted.reshape(SLOTS)


def solution(mesh):
    finer = Mesh(mesh.devices.reshape(NX, NZ, NY, NC), ("x", "z", "y", "c"))
    every = ("x", "z", "y", "c")
    placed = (P(DP, None, VOCAB), P(None, every), P(DP, None), P(DP, None), P(DP, None), P())

    return jax.shard_map(
        local, mesh=finer, in_specs=placed, out_specs=(P(DP, None), P(DP), P(DP)), check_vma=False
    )
```

```python
import jax
import jax.numpy as jnp
from jax import lax
from jax.experimental import pallas as pl
from jax.experimental.pallas import tpu as pltpu
from jax.sharding import Mesh
from jax.sharding import PartitionSpec as P


SAMPLES = 8
DP = ("x", "z")
VOCAB = ("y", "c")
REWARD_UNIT = 1.0 / 64.0
NX, NZ, NY, NC = 4, 8, 4, 2
SLOTS, WINDOW, WIDTH = 8, 14, 512
HALF = 28
MSG = 32
ROWS = NZ * HALF
META = NZ
SHARD = 501
TALL = ROWS + META
OFFSETS = (0, -1, 1, 2)
F32 = jnp.float32
BF16 = jnp.bfloat16
VMEM = pl.BlockSpec(memory_space=pltpu.VMEM)
SMEM = pl.BlockSpec(memory_space=pltpu.SMEM)
HBM = pl.BlockSpec(memory_space=pltpu.HBM)


def params(mib=32):
    return pltpu.CompilerParams(vmem_limit_bytes=mib * 2**20)


def in_hbm(*arrays):
    return [pltpu.with_memory_space_constraint(a, pltpu.HBM) for a in arrays]


def shift(value, axis, by):
    size = lax.axis_size(axis)
    return lax.ppermute(value, axis, [(i, (i + by) % size) for i in range(size)])


def pack_kernel(hidden_hbm, targets_hbm, lengths_hbm, rewards_hbm, out, hidden, targets, lengths, rewards, sems):
    copies = [
        pltpu.make_async_copy(src, dst, sems.at[k])
        for k, (src, dst) in enumerate(
            (
                (lengths_hbm, lengths),
                (rewards_hbm, rewards),
                (targets_hbm, targets),
                (hidden_hbm, hidden),
            )
        )
    ]
    for copy in copies:
        copy.start()
    for copy in copies:
        copy.wait()
    lane = lax.broadcasted_iota(jnp.int32, (1, 128), 1)
    offsets, both = [], jnp.zeros((1, 128), jnp.int32)
    offset_of = jnp.zeros((MSG, SLOTS), jnp.int32)
    length_of = jnp.zeros((MSG, SLOTS), jnp.int32)
    slot = lax.broadcasted_iota(jnp.int32, (MSG, SLOTS), 1)
    at = jnp.int32(0)
    for g in range(SLOTS):
        offsets.append(at)
        offset_of = jnp.where(slot == g, at, offset_of)
        length_of = jnp.where(slot == g, lengths[0, g], length_of)
        both = jnp.where(lane == g, lengths[0, g], both)
        both = jnp.where(lane == SLOTS + g, rewards[0, g], both)
        at = at + lengths[0, g]
    row_of = lax.broadcasted_iota(jnp.int32, (MSG, SLOTS), 0)
    row = lax.broadcasted_iota(jnp.int32, (MSG, WINDOW), 0)
    step = lax.broadcasted_iota(jnp.int32, (MSG, WINDOW), 1)
    wanted = targets[...]
    digits = [(wanted & 255), (wanted >> 8) & 255, wanted >> 16]
    out_row = lax.broadcasted_iota(jnp.int32, (MSG, WIDTH), 0)
    for half in range(NC):
        rows = jnp.zeros((MSG, WIDTH), F32)
        for t in range(WINDOW):
            here = (row_of + half * HALF == offset_of + t) & (t < length_of) & (row_of < HALF)
            chooser = jnp.where(here, 1.0, 0.0).astype(BF16)
            rows += jnp.dot(chooser, hidden[t], preferred_element_type=F32)
        ids = jnp.zeros((8, MSG), F32)
        for g in range(SLOTS):
            here = (row + half * HALF == offsets[g] + step) & (step < lengths[0, g]) & (row < HALF)
            chooser = jnp.where(here, 1.0, 0.0).astype(BF16)
            three = jnp.concatenate(
                [d[g : g + 1, :] for d in digits] + [jnp.zeros((5, WINDOW), jnp.int32)], axis=0
            )
            ids += lax.dot_general(
                three.astype(F32).astype(BF16),
                chooser,
                (((1,), (1,)), ((), ())),
                preferred_element_type=F32,
            )
        pad = jnp.zeros((1, 128 - MSG), F32)
        meta = jnp.concatenate(
            [ids[0:1], pad, ids[1:2], pad, ids[2:3], pad, both.astype(F32)], axis=1
        )
        message = jnp.where(out_row == HALF, meta, rows).astype(BF16)
        for z in range(NZ):
            out[z * NC + half] = message


def unpack_kernel(got, first, second):
    for core, out in enumerate((first, second)):
        pieces = [got[z * NC + core].astype(F32)[:HALF] for z in range(NZ)]
        if core == 0:
            pieces += [got[z * NC].astype(F32)[HALF : HALF + 1] for z in range(NZ)]
        out[...] = jnp.concatenate(pieces, axis=0).astype(BF16)


def join_kernel(one, two, out):
    out[: one.shape[0]] = one[...]
    out[one.shape[0] :] = two[...]


def join(one, two):
    return pl.pallas_call(
        join_kernel,
        out_shape=jax.ShapeDtypeStruct((one.shape[0] + two.shape[0], one.shape[1]), BF16),
        in_specs=[VMEM, VMEM],
        out_specs=VMEM,
        compiler_params=params(),
    )(one, two)


def gathered_planes(own, firsts, lasts):
    both = range(2)
    up = [shift(own[k], firsts[k], 1) for k in both]
    down = [shift(own[k], firsts[k], -1) for k in both]
    far = [shift(up[k], firsts[k], 1) for k in both]
    one = [join(own[k], up[k]) for k in both]
    two = [join(down[k], far[k]) for k in both]
    planes = []
    for k in both:
        up1 = shift(one[k], lasts[k], 1)
        down1 = shift(one[k], lasts[k], -1)
        down2 = shift(two[k], lasts[k], -1)
        up2 = shift(two[k], lasts[k], 1)
        far2 = shift(down2, lasts[k], -1)
        far1 = shift(up1, lasts[k], 1)
        planes.append(((one[k], two[k]), (up1, up2), (down1, down2), (far1, far2)))
    return planes


def product(w, block):
    return lax.dot_general(w[...], block, (((1,), (1,)), ((), ())), preferred_element_type=F32)


LOOK = 4


class Arrivals:
    def __init__(self):
        self.order, self.copies, self.begun = [], {}, 0

    def add(self, key, *copies):
        if key not in self.copies:
            self.order.append(key)
            self.copies[key] = copies

    def begin(self, upto):
        while self.begun < min(upto, len(self.order)):
            for copy in self.copies[self.order[self.begun]]:
                copy.start()
            self.begun += 1

    def wait(self, key):
        if self.copies.get(key):
            self.begin(self.order.index(key) + 1 + LOOK)
            for copy in self.copies[key]:
                copy.wait()
            self.copies[key] = ()


def names_of(which):
    return [(k, j, part) for k in range(2) for j in which for part in range(2)]


def plan_of(which):
    plan = []
    for i in [i for i in range(NX) if i not in which] + list(which):
        terms = [((j, 0), (0, j, i // 2), i % 2 * TALL) for j in which]
        if i in which:
            terms += [((j, 1), (1, i, j // 2), j % 2 * ROWS) for j in range(NY)]
        plan.append((i, terms))
    return plan


NEAR, FAR = (0, 1, 2), (3,)
KEPT = tuple((j, 1) for j in range(NY)) + ((3, 0),)
NEAR_LATE = [n for n in names_of(NEAR) if n[1] and n[1] - 1 != n[2]]
FAR_LATE = names_of(FAR)


def piece_copies(arrivals, name, pieces, late, held_p, sems):
    ref = pieces[name]
    if name not in late:
        return ref
    n = late.index(name)
    arrivals.add(name, pltpu.make_async_copy(ref, held_p.at[n, pl.ds(0, ref.shape[0])], sems.at[n]))
    return held_p.at[n]


def near_kernel(at, *refs):
    pieces = dict(zip(names_of(NEAR), refs))
    weights, rest = refs[len(pieces) : len(pieces) + 2], refs[len(pieces) + 2 :]
    acc, kept, held_p, held_w, sems, sems_w = rest
    arrivals, views, slices = Arrivals(), {}, {}

    def slice_copies(key):
        j, colour = key
        if key in KEPT:
            slices[key] = kept.at[KEPT.index(key)]
        else:
            slices[key] = held_w.at[j]
        column = ((at[0] + OFFSETS[j] + NY) % NY * NC + colour) * WIDTH
        column = pl.multiple_of(column, WIDTH)
        arrivals.add(
            key,
            *(
                pltpu.make_async_copy(
                    weights[w].at[:, pl.ds(column, WIDTH)], slices[key].at[w], sems_w.at[j, colour, w]
                )
                for w in range(2)
            ),
        )

    plan = plan_of(NEAR)
    for _, terms in plan:
        for key, name, _ in terms:
            if key not in slices:
                slice_copies(key)
            if name not in views:
                views[name] = piece_copies(arrivals, name, pieces, NEAR_LATE, held_p, sems)
    slice_copies((3, 0))
    arrivals.begin(LOOK)
    for i, terms in plan:
        total = [None, None]
        for key, name, lo in terms:
            arrivals.wait(key)
            arrivals.wait(name)
            for w in range(2):
                term = product(slices[key].at[w], views[name][lo : lo + ROWS, :])
                total[w] = term if total[w] is None else total[w] + term
        for w in range(2):
            acc[i, w] = total[w]
    arrivals.wait((3, 0))


def far_kernel(at, *refs):
    pieces = dict(zip(names_of(FAR), refs))
    before, kept, ids, out, acc, held, held_p, sems = refs[len(pieces) :]
    arrivals, views = Arrivals(), {}
    plan = plan_of(FAR)
    for _, terms in plan:
        for _, name, _ in terms:
            if name not in views:
                views[name] = piece_copies(arrivals, name, pieces, FAR_LATE, held_p, sems)
    arrivals.begin(LOOK)
    for i, terms in plan:
        total = [before[i, w] for w in range(2)]
        for key, name, lo in terms:
            arrivals.wait(name)
            for w in range(2):
                total[w] = total[w] + product(kept.at[KEPT.index(key), w], views[name][lo : lo + ROWS, :])
        for w in range(2):
            acc[i, w] = total[w]
    statistics(at, ids, acc, out, held)


def statistics(at, ids, acc, out, held):
    x = at[1]
    held[...] = jnp.zeros_like(held)
    column = lax.broadcasted_iota(jnp.int32, (SHARD, ROWS), 0)
    for i in range(NX):
        own, other = acc[i, 0], acc[i, 1]
        top = jnp.maximum(jnp.max(own, 0, keepdims=True), jnp.max(other, 0, keepdims=True))
        total = jnp.sum(jnp.exp(own - top), 0, keepdims=True) + jnp.sum(
            jnp.exp(other - top), 0, keepdims=True
        )
        wanted = ids[i : i + 1, :ROWS]
        hit = jnp.sum(jnp.where(column == wanted - at[2], own, 0.0), 0, keepdims=True)
        hit += jnp.sum(jnp.where(column == wanted - at[3], other, 0.0), 0, keepdims=True)
        x_at = (x + OFFSETS[i] + NX) % NX
        held[pl.ds(x_at, 1), :ROWS] = top + jnp.log(total)
        held[pl.ds(4 + x_at, 1), :ROWS] = hit
    for k in range(out.shape[0]):
        out[k] = held[...]


def head(at, planes, weights, ids):
    acc = pltpu.VMEM((NX, 2, SHARD, ROWS), F32)
    kept = pltpu.VMEM((len(KEPT), 2, SHARD, WIDTH), BF16)

    def operands(which, late):
        parts, specs = [], []
        for name in names_of(which):
            piece = planes[name[0]][name[1]][name[2]]
            parts += in_hbm(piece) if name in late else [piece]
            specs.append(HBM if name in late else VMEM)
        return parts, specs

    parts, specs = operands(NEAR, NEAR_LATE)
    sums, slices = pl.pallas_call(
        near_kernel,
        out_shape=[acc, kept],
        in_specs=[SMEM] + specs + [HBM] * 2,
        out_specs=[VMEM, VMEM],
        scratch_shapes=[
            pltpu.VMEM((len(NEAR_LATE), 2 * TALL, WIDTH), BF16),
            pltpu.VMEM((len(NEAR), 2, SHARD, WIDTH), BF16),
            pltpu.SemaphoreType.DMA((len(NEAR_LATE),)),
            pltpu.SemaphoreType.DMA((NY, NC, 2)),
        ],
        compiler_params=params(24),
    )(at, *parts, *weights)
    parts, specs = operands(FAR, FAR_LATE)
    return pl.pallas_call(
        far_kernel,
        out_shape=jax.ShapeDtypeStruct((NX * NY, 8, 256), F32),
        in_specs=[SMEM] + specs + [VMEM] * 3,
        out_specs=VMEM,
        scratch_shapes=[
            acc,
            pltpu.VMEM((8, 256), F32),
            pltpu.VMEM((len(FAR_LATE), 2 * TALL, WIDTH), BF16),
            pltpu.SemaphoreType.DMA((len(FAR_LATE),)),
        ],
        compiler_params=params(24),
    )(at, *parts, sums, slices, ids)


def merged_parts(parts):
    top, hit = parts[0][:4], parts[0][4:]
    for part in parts[1:]:
        top = jnp.maximum(top, part[:4])
        hit = hit + part[4:]
    total = jnp.zeros_like(top)
    for part in parts:
        total = total + jnp.exp(part[:4] - top)
    return top + jnp.log(total), hit


def merge_kernel(parts, out):
    lse, hit = merged_parts([parts[k] for k in range(parts.shape[0])])
    for k in range(out.shape[0]):
        out[k, :4] = lse
        out[k, 4:] = hit


def final_kernel(parts, source, reward, length, logprobs, advantage, weighted):
    tables = []
    for core in range(NC):
        lse, hit = merged_parts([parts[z * NC + core] for z in range(NZ)])
        tables.append(hit - lse)
    lane = lax.broadcasted_iota(jnp.int32, (SLOTS, 256), 1)
    wanted = source[...]
    total = jnp.zeros((SLOTS, 1), F32)
    columns = []
    for t in range(WINDOW):
        at = wanted[:, t : t + 1]
        found = jnp.zeros((SLOTS, 256), F32)
        for core in range(NC):
            for x in range(NX):
                here = at - (core * NX + x) * 256 == lane
                found = jnp.where(here, tables[core][x : x + 1, :], found)
        value = jnp.sum(found, axis=1, keepdims=True)
        columns.append(value)
        total = total + value
    logprobs[...] = jnp.concatenate(columns, axis=1)
    row = lax.broadcasted_iota(jnp.int32, (SLOTS, SLOTS), 0)
    across = lax.broadcasted_iota(jnp.int32, (SLOTS, SLOTS), 1)
    line = jnp.sum(jnp.where(row == across, total, 0.0), axis=0, keepdims=True)
    own = reward[...].astype(F32) * REWARD_UNIT
    spare = own - (jnp.sum(own, axis=1, keepdims=True) - own) / (SAMPLES - 1.0)
    advantage[...] = spare
    weighted[...] = spare * line / length[...].astype(F32)


def local(hidden, weight, targets, lengths, rewards, arrival):
    shard = weight.shape[1]
    x, z, y, c = (lax.axis_index(a) for a in ("x", "z", "y", "c"))
    swapped = shift(weight, "c", 1)
    sent = pl.pallas_call(
        pack_kernel,
        out_shape=pltpu.VMEM((NZ * NC, MSG, WIDTH), BF16),
        in_specs=[HBM] * 4,
        out_specs=VMEM,
        scratch_shapes=[
            pltpu.VMEM((WINDOW, SLOTS, WIDTH), BF16),
            pltpu.VMEM((SLOTS, WINDOW), jnp.int32),
            pltpu.SMEM((1, SLOTS), jnp.int32),
            pltpu.SMEM((1, SLOTS), jnp.int32),
            pltpu.SemaphoreType.DMA((4,)),
        ],
        compiler_params=params(),
    )(*in_hbm(hidden.transpose(1, 0, 2), targets, lengths, rewards))
    got = lax.all_to_all(sent, ("z", "c"), 0, 0, tiled=True)
    own0, own1 = pl.pallas_call(
        unpack_kernel,
        out_shape=[
            jax.ShapeDtypeStruct((TALL, WIDTH), BF16),
            jax.ShapeDtypeStruct((ROWS, WIDTH), BF16),
        ],
        in_specs=[VMEM],
        out_specs=[VMEM, VMEM],
        compiler_params=params(),
    )(got)
    planes = gathered_planes((own0, own1), ("x", "y"), ("y", "x"))
    line0 = planes[0][0]

    metas = jnp.stack([line0[i // 2][i % 2 * TALL + ROWS : i % 2 * TALL + TALL] for i in range(NX)])
    whole = metas.astype(F32).astype(jnp.int32)
    ids = whole[:, :, :HALF] + 256 * whole[:, :, 128 : 128 + HALF] + 65536 * whole[:, :, 256 : 256 + HALF]
    ids = jnp.pad(ids.reshape(NX, ROWS), ((0, 4), (0, 0)), constant_values=-1)

    dp = x * NZ + z
    base = (dp * NY + y) * NC
    at = jnp.stack([y, x, (base + c) * shard, (base + 1 - c) * shard]).astype(jnp.int32)
    partial = head(at, planes, in_hbm(weight.T, swapped.T), ids)

    order = (lax.iota(jnp.int32, NX) - x + NX) % NX
    relative = jnp.where(order == 0, 0, jnp.where(order == 3, 1, order + 1))
    per_slot = jnp.sum(
        jnp.where(
            (relative[:, None] == lax.iota(jnp.int32, NX)[None, :])[:, :, None, None],
            whole[None, :, :, 384 : 384 + 2 * SLOTS],
            0,
        ),
        axis=1,
    ).reshape(NX * NZ, 2 * SLOTS)
    all_lengths, all_rewards = per_slot[:, :SLOTS], per_slot[:, SLOTS:]
    count = NX * NZ * SLOTS
    slot_ids = lax.iota(jnp.int32, count)
    mine = lax.iota(jnp.int32, SLOTS) + dp * SLOTS
    matching = arrival[None, :] == mine[:, None]

    def lookup(table):
        return jnp.sum(jnp.where(matching, table.reshape(count)[None, :], 0), axis=1)

    slot_of = lookup(slot_ids)
    length_of = lookup(all_lengths)
    reward_of = lookup(all_rewards)
    offset_of = lookup(jnp.cumsum(all_lengths, axis=1) - all_lengths)
    group = slot_of // SLOTS
    line = offset_of[:, None] + lax.iota(jnp.int32, WINDOW)[None, :]
    usable = lax.iota(jnp.int32, WINDOW)[None, :] < length_of[:, None]
    place = group // NZ * 256 + group % NZ * HALF
    source = jnp.where(usable, place[:, None] + line // HALF * 1024 + line % HALF, -1)

    stats = lax.all_to_all(partial, ("x", "y"), 0, 0, tiled=True)
    stats = pl.pallas_call(
        merge_kernel,
        out_shape=pltpu.VMEM((NZ * NC, 8, 256), F32),
        in_specs=[VMEM],
        out_specs=VMEM,
        compiler_params=params(),
    )(stats)
    stats = lax.all_to_all(stats, ("z", "c"), 0, 0, tiled=True)
    token_logprobs, advantages, weighted = pl.pallas_call(
        final_kernel,
        out_shape=[
            jax.ShapeDtypeStruct((SLOTS, WINDOW), F32),
            jax.ShapeDtypeStruct((1, SLOTS), F32),
            jax.ShapeDtypeStruct((1, SLOTS), F32),
        ],
        in_specs=[VMEM] * 4,
        out_specs=[VMEM] * 3,
        compiler_params=params(),
    )(stats, source, reward_of[None, :], length_of[None, :])
    return token_logprobs, advantages.reshape(SLOTS), weighted.reshape(SLOTS)


def solution(mesh):
    finer = Mesh(mesh.devices.reshape(NX, NZ, NY, NC), ("x", "z", "y", "c"))
    every = ("x", "z", "y", "c")
    placed = (P(DP, None, VOCAB), P(None, every), P(DP, None), P(DP, None), P(DP, None), P())

    return jax.shard_map(
        local, mesh=finer, in_specs=placed, out_specs=(P(DP, None), P(DP), P(DP)), check_vma=False
    )
```

```python
import jax
import jax.numpy as jnp
from jax import lax
from jax.experimental import pallas as pl
from jax.experimental.pallas import tpu as pltpu
from jax.sharding import Mesh
from jax.sharding import PartitionSpec as P


SAMPLES = 8
DP = ("x", "z")
VOCAB = ("y", "c")
REWARD_UNIT = 1.0 / 64.0
NX, NZ, NY, NC = 4, 8, 4, 2
SLOTS, WINDOW, WIDTH = 8, 14, 512
HALF = 28
MSG = 32
ROWS = NZ * HALF
META = NZ
SHARD = 501
TALL = ROWS + META
OFFSETS = (0, -1, 1, 2)
F32 = jnp.float32
BF16 = jnp.bfloat16
VMEM = pl.BlockSpec(memory_space=pltpu.VMEM)
SMEM = pl.BlockSpec(memory_space=pltpu.SMEM)
HBM = pl.BlockSpec(memory_space=pltpu.HBM)


def params(mib=32):
    return pltpu.CompilerParams(vmem_limit_bytes=mib * 2**20)


def in_hbm(*arrays):
    return [pltpu.with_memory_space_constraint(a, pltpu.HBM) for a in arrays]


def shift(value, axis, by):
    size = lax.axis_size(axis)
    return lax.ppermute(value, axis, [(i, (i + by) % size) for i in range(size)])


def pack_kernel(hidden_hbm, targets_hbm, lengths_hbm, rewards_hbm, out, hidden, targets, lengths, rewards, sems):
    copies = [
        pltpu.make_async_copy(src, dst, sems.at[k])
        for k, (src, dst) in enumerate(
            (
                (lengths_hbm, lengths),
                (rewards_hbm, rewards),
                (targets_hbm, targets),
                (hidden_hbm, hidden),
            )
        )
    ]
    for copy in copies:
        copy.start()
    for copy in copies:
        copy.wait()
    lane = lax.broadcasted_iota(jnp.int32, (1, 128), 1)
    offsets, both = [], jnp.zeros((1, 128), jnp.int32)
    offset_of = jnp.zeros((MSG, SLOTS), jnp.int32)
    length_of = jnp.zeros((MSG, SLOTS), jnp.int32)
    slot = lax.broadcasted_iota(jnp.int32, (MSG, SLOTS), 1)
    at = jnp.int32(0)
    for g in range(SLOTS):
        offsets.append(at)
        offset_of = jnp.where(slot == g, at, offset_of)
        length_of = jnp.where(slot == g, lengths[0, g], length_of)
        both = jnp.where(lane == g, lengths[0, g], both)
        both = jnp.where(lane == SLOTS + g, rewards[0, g], both)
        at = at + lengths[0, g]
    row_of = lax.broadcasted_iota(jnp.int32, (MSG, SLOTS), 0)
    row = lax.broadcasted_iota(jnp.int32, (MSG, WINDOW), 0)
    step = lax.broadcasted_iota(jnp.int32, (MSG, WINDOW), 1)
    wanted = targets[...]
    digits = [(wanted & 255), (wanted >> 8) & 255, wanted >> 16]
    out_row = lax.broadcasted_iota(jnp.int32, (MSG, WIDTH), 0)
    for half in range(NC):
        rows = jnp.zeros((MSG, WIDTH), F32)
        for t in range(WINDOW):
            here = (row_of + half * HALF == offset_of + t) & (t < length_of) & (row_of < HALF)
            chooser = jnp.where(here, 1.0, 0.0).astype(BF16)
            rows += jnp.dot(chooser, hidden[t], preferred_element_type=F32)
        ids = jnp.zeros((8, MSG), F32)
        for g in range(SLOTS):
            here = (row + half * HALF == offsets[g] + step) & (step < lengths[0, g]) & (row < HALF)
            chooser = jnp.where(here, 1.0, 0.0).astype(BF16)
            three = jnp.concatenate(
                [d[g : g + 1, :] for d in digits] + [jnp.zeros((5, WINDOW), jnp.int32)], axis=0
            )
            ids += lax.dot_general(
                three.astype(F32).astype(BF16),
                chooser,
                (((1,), (1,)), ((), ())),
                preferred_element_type=F32,
            )
        pad = jnp.zeros((1, 128 - MSG), F32)
        meta = jnp.concatenate(
            [ids[0:1], pad, ids[1:2], pad, ids[2:3], pad, both.astype(F32)], axis=1
        )
        message = jnp.where(out_row == HALF, meta, rows).astype(BF16)
        for z in range(NZ):
            out[z * NC + half] = message


def unpack_kernel(got, first, second):
    for core, out in enumerate((first, second)):
        pieces = [got[z * NC + core].astype(F32)[:HALF] for z in range(NZ)]
        if core == 0:
            pieces += [got[z * NC].astype(F32)[HALF : HALF + 1] for z in range(NZ)]
        out[...] = jnp.concatenate(pieces, axis=0).astype(BF16)


def join_kernel(one, two, out):
    out[: one.shape[0]] = one[...]
    out[one.shape[0] :] = two[...]


def join(one, two):
    return pl.pallas_call(
        join_kernel,
        out_shape=jax.ShapeDtypeStruct((one.shape[0] + two.shape[0], one.shape[1]), BF16),
        in_specs=[VMEM, VMEM],
        out_specs=VMEM,
        compiler_params=params(),
    )(one, two)


def gathered_planes(own, firsts, lasts):
    both = range(2)
    up = [shift(own[k], firsts[k], 1) for k in both]
    down = [shift(own[k], firsts[k], -1) for k in both]
    far = [shift(up[k], firsts[k], 1) for k in both]
    one, two = [], []
    for k in both:
        one.append(join(own[k], up[k]))
        two.append(join(down[k], far[k]))
    planes = []
    for k in both:
        up1 = shift(one[k], lasts[k], 1)
        down1 = shift(one[k], lasts[k], -1)
        down2 = shift(two[k], lasts[k], -1)
        up2 = shift(two[k], lasts[k], 1)
        far2 = shift(down2, lasts[k], -1)
        far1 = shift(up1, lasts[k], 1)
        planes.append(((one[k], two[k]), (up1, up2), (down1, down2), (far1, far2)))
    return planes


def product(w, block):
    return lax.dot_general(w[...], block, (((1,), (1,)), ((), ())), preferred_element_type=F32)


LOOK = 4


class Arrivals:
    def __init__(self):
        self.order, self.copies, self.begun = [], {}, 0

    def add(self, key, *copies):
        if key not in self.copies:
            self.order.append(key)
            self.copies[key] = copies

    def begin(self, upto):
        while self.begun < min(upto, len(self.order)):
            for copy in self.copies[self.order[self.begun]]:
                copy.start()
            self.begun += 1

    def wait(self, key):
        if self.copies.get(key):
            self.begin(self.order.index(key) + 1 + LOOK)
            for copy in self.copies[key]:
                copy.wait()
            self.copies[key] = ()


def names_of(which):
    return [(k, j, part) for k in range(2) for j in which for part in range(2)]


def plan_of(which):
    plan = []
    for i in [i for i in range(NX) if i not in which] + list(which):
        terms = [((j, 0), (0, j, i // 2), i % 2 * TALL) for j in which]
        if i in which:
            terms += [((j, 1), (1, i, j // 2), j % 2 * ROWS) for j in range(NY)]
        plan.append((i, terms))
    return plan


NEAR, FAR = (0, 1, 2), (3,)
KEPT = tuple((j, 1) for j in range(NY)) + ((3, 0),)
NEAR_LATE = [n for n in names_of(NEAR) if n[1] and n[1] - 1 != n[2]]


def piece_copies(arrivals, name, pieces, late, held_p, sems):
    ref = pieces[name]
    if name not in late:
        return ref
    n = late.index(name)
    arrivals.add(name, pltpu.make_async_copy(ref, held_p.at[n, pl.ds(0, ref.shape[0])], sems.at[n]))
    return held_p.at[n]


def near_kernel(at, *refs):
    pieces = dict(zip(names_of(NEAR), refs))
    weights, rest = refs[len(pieces) : len(pieces) + 2], refs[len(pieces) + 2 :]
    acc, kept, held_p, held_w, sems, sems_w = rest
    arrivals, views, slices = Arrivals(), {}, {}

    def slice_copies(key):
        j, colour = key
        if key in KEPT:
            slices[key] = kept.at[KEPT.index(key)]
        else:
            slices[key] = held_w.at[j]
        column = ((at[0] + OFFSETS[j] + NY) % NY * NC + colour) * WIDTH
        column = pl.multiple_of(column, WIDTH)
        arrivals.add(
            key,
            *(
                pltpu.make_async_copy(
                    weights[w].at[:, pl.ds(column, WIDTH)], slices[key].at[w], sems_w.at[j, colour, w]
                )
                for w in range(2)
            ),
        )

    plan = plan_of(NEAR)
    for _, terms in plan:
        for key, name, _ in terms:
            if key not in slices:
                slice_copies(key)
            if name not in views:
                views[name] = piece_copies(arrivals, name, pieces, NEAR_LATE, held_p, sems)
    slice_copies((3, 0))
    arrivals.begin(LOOK)
    for i, terms in plan:
        total = [None, None]
        for key, name, lo in terms:
            arrivals.wait(key)
            arrivals.wait(name)
            for w in range(2):
                term = product(slices[key].at[w], views[name][lo : lo + ROWS, :])
                total[w] = term if total[w] is None else total[w] + term
        for w in range(2):
            acc[i, w] = total[w]
    arrivals.wait((3, 0))


def far_kernel(at, *refs):
    pieces = dict(zip(names_of(FAR), refs))
    before, kept, ids, out, acc, held = refs[len(pieces) :]
    for i, terms in plan_of(FAR):
        total = [before[i, w] for w in range(2)]
        for key, name, lo in terms:
            for w in range(2):
                total[w] = total[w] + product(kept.at[KEPT.index(key), w], pieces[name][lo : lo + ROWS, :])
        for w in range(2):
            acc[i, w] = total[w]
    statistics(at, ids, acc, out, held)


def statistics(at, ids, acc, out, held):
    x = at[1]
    held[...] = jnp.zeros_like(held)
    column = lax.broadcasted_iota(jnp.int32, (SHARD, ROWS), 0)
    for i in range(NX):
        own, other = acc[i, 0], acc[i, 1]
        top = jnp.maximum(jnp.max(own, 0, keepdims=True), jnp.max(other, 0, keepdims=True))
        total = jnp.sum(jnp.exp(own - top), 0, keepdims=True) + jnp.sum(
            jnp.exp(other - top), 0, keepdims=True
        )
        wanted = ids[i : i + 1, :ROWS]
        hit = jnp.sum(jnp.where(column == wanted - at[2], own, 0.0), 0, keepdims=True)
        hit += jnp.sum(jnp.where(column == wanted - at[3], other, 0.0), 0, keepdims=True)
        x_at = (x + OFFSETS[i] + NX) % NX
        held[pl.ds(x_at, 1), :ROWS] = top + jnp.log(total)
        held[pl.ds(4 + x_at, 1), :ROWS] = hit
    for k in range(out.shape[0]):
        out[k] = held[...]


def head(at, planes, weights, ids):
    acc = pltpu.VMEM((NX, 2, SHARD, ROWS), F32)
    kept = pltpu.VMEM((len(KEPT), 2, SHARD, WIDTH), BF16)

    def operands(which, late=()):
        parts, specs = [], []
        for name in names_of(which):
            piece = planes[name[0]][name[1]][name[2]]
            parts += in_hbm(piece) if name in late else [piece]
            specs.append(HBM if name in late else VMEM)
        return parts, specs

    parts, specs = operands(NEAR, NEAR_LATE)
    sums, slices = pl.pallas_call(
        near_kernel,
        out_shape=[acc, kept],
        in_specs=[SMEM] + specs + [HBM] * 2,
        out_specs=[VMEM, VMEM],
        scratch_shapes=[
            pltpu.VMEM((len(NEAR_LATE), 2 * TALL, WIDTH), BF16),
            pltpu.VMEM((len(NEAR), 2, SHARD, WIDTH), BF16),
            pltpu.SemaphoreType.DMA((len(NEAR_LATE),)),
            pltpu.SemaphoreType.DMA((NY, NC, 2)),
        ],
        compiler_params=params(24),
    )(at, *parts, *weights)
    parts, specs = operands(FAR)
    return pl.pallas_call(
        far_kernel,
        out_shape=jax.ShapeDtypeStruct((NX * NY, 8, 256), F32),
        in_specs=[SMEM] + specs + [VMEM] * 3,
        out_specs=VMEM,
        scratch_shapes=[acc, pltpu.VMEM((8, 256), F32)],
        compiler_params=params(24),
    )(at, *parts, sums, slices, ids)


def merged_parts(parts):
    top, hit = parts[0][:4], parts[0][4:]
    for part in parts[1:]:
        top = jnp.maximum(top, part[:4])
        hit = hit + part[4:]
    total = jnp.zeros_like(top)
    for part in parts:
        total = total + jnp.exp(part[:4] - top)
    return top + jnp.log(total), hit


def merge_kernel(parts, out):
    lse, hit = merged_parts([parts[k] for k in range(parts.shape[0])])
    for k in range(out.shape[0]):
        out[k, :4] = lse
        out[k, 4:] = hit


def final_kernel(parts, source, reward, length, logprobs, advantage, weighted):
    tables = []
    for core in range(NC):
        lse, hit = merged_parts([parts[z * NC + core] for z in range(NZ)])
        tables.append(hit - lse)
    lane = lax.broadcasted_iota(jnp.int32, (SLOTS, 256), 1)
    wanted = source[...]
    total = jnp.zeros((SLOTS, 1), F32)
    columns = []
    for t in range(WINDOW):
        at = wanted[:, t : t + 1]
        found = jnp.zeros((SLOTS, 256), F32)
        for core in range(NC):
            for x in range(NX):
                here = at - (core * NX + x) * 256 == lane
                found = jnp.where(here, tables[core][x : x + 1, :], found)
        value = jnp.sum(found, axis=1, keepdims=True)
        columns.append(value)
        total = total + value
    logprobs[...] = jnp.concatenate(columns, axis=1)
    row = lax.broadcasted_iota(jnp.int32, (SLOTS, SLOTS), 0)
    across = lax.broadcasted_iota(jnp.int32, (SLOTS, SLOTS), 1)
    line = jnp.sum(jnp.where(row == across, total, 0.0), axis=0, keepdims=True)
    own = reward[...].astype(F32) * REWARD_UNIT
    spare = own - (jnp.sum(own, axis=1, keepdims=True) - own) / (SAMPLES - 1.0)
    advantage[...] = spare
    weighted[...] = spare * line / length[...].astype(F32)


def local(hidden, weight, targets, lengths, rewards, arrival):
    shard = weight.shape[1]
    x, z, y, c = (lax.axis_index(a) for a in ("x", "z", "y", "c"))
    swapped = shift(weight, "c", 1)
    sent = pl.pallas_call(
        pack_kernel,
        out_shape=pltpu.VMEM((NZ * NC, MSG, WIDTH), BF16),
        in_specs=[HBM] * 4,
        out_specs=VMEM,
        scratch_shapes=[
            pltpu.VMEM((WINDOW, SLOTS, WIDTH), BF16),
            pltpu.VMEM((SLOTS, WINDOW), jnp.int32),
            pltpu.SMEM((1, SLOTS), jnp.int32),
            pltpu.SMEM((1, SLOTS), jnp.int32),
            pltpu.SemaphoreType.DMA((4,)),
        ],
        compiler_params=params(),
    )(*in_hbm(hidden.transpose(1, 0, 2), targets, lengths, rewards))
    got = lax.all_to_all(sent, ("z", "c"), 0, 0, tiled=True)
    own0, own1 = pl.pallas_call(
        unpack_kernel,
        out_shape=[
            jax.ShapeDtypeStruct((TALL, WIDTH), BF16),
            jax.ShapeDtypeStruct((ROWS, WIDTH), BF16),
        ],
        in_specs=[VMEM],
        out_specs=[VMEM, VMEM],
        compiler_params=params(),
    )(got)
    planes = gathered_planes((own0, own1), ("x", "y"), ("y", "x"))
    line0 = planes[0][0]

    metas = jnp.stack([line0[i // 2][i % 2 * TALL + ROWS : i % 2 * TALL + TALL] for i in range(NX)])
    whole = metas.astype(F32).astype(jnp.int32)
    ids = whole[:, :, :HALF] + 256 * whole[:, :, 128 : 128 + HALF] + 65536 * whole[:, :, 256 : 256 + HALF]
    ids = jnp.pad(ids.reshape(NX, ROWS), ((0, 4), (0, 0)), constant_values=-1)

    dp = x * NZ + z
    base = (dp * NY + y) * NC
    at = jnp.stack([y, x, (base + c) * shard, (base + 1 - c) * shard]).astype(jnp.int32)

    order = (lax.iota(jnp.int32, NX) - x + NX) % NX
    relative = jnp.where(order == 0, 0, jnp.where(order == 3, 1, order + 1))
    per_slot = jnp.sum(
        jnp.where(
            (relative[:, None] == lax.iota(jnp.int32, NX)[None, :])[:, :, None, None],
            whole[None, :, :, 384 : 384 + 2 * SLOTS],
            0,
        ),
        axis=1,
    ).reshape(NX * NZ, 2 * SLOTS)
    all_lengths, all_rewards = per_slot[:, :SLOTS], per_slot[:, SLOTS:]
    count = NX * NZ * SLOTS
    slot_ids = lax.iota(jnp.int32, count)
    mine = lax.iota(jnp.int32, SLOTS) + dp * SLOTS
    matching = arrival[None, :] == mine[:, None]

    def lookup(table):
        return jnp.sum(jnp.where(matching, table.reshape(count)[None, :], 0), axis=1)

    slot_of = lookup(slot_ids)
    length_of = lookup(all_lengths)
    reward_of = lookup(all_rewards)
    offset_of = lookup(jnp.cumsum(all_lengths, axis=1) - all_lengths)
    group = slot_of // SLOTS
    line = offset_of[:, None] + lax.iota(jnp.int32, WINDOW)[None, :]
    usable = lax.iota(jnp.int32, WINDOW)[None, :] < length_of[:, None]
    place = group // NZ * 256 + group % NZ * HALF
    source = jnp.where(usable, place[:, None] + line // HALF * 1024 + line % HALF, -1)

    partial = head(at, planes, in_hbm(weight.T, swapped.T), ids)

    stats = lax.all_to_all(partial, ("x", "y"), 0, 0, tiled=True)
    stats = pl.pallas_call(
        merge_kernel,
        out_shape=pltpu.VMEM((NZ * NC, 8, 256), F32),
        in_specs=[VMEM],
        out_specs=VMEM,
        compiler_params=params(),
    )(stats)
    stats = lax.all_to_all(stats, ("z", "c"), 0, 0, tiled=True)
    token_logprobs, advantages, weighted = pl.pallas_call(
        final_kernel,
        out_shape=[
            jax.ShapeDtypeStruct((SLOTS, WINDOW), F32),
            jax.ShapeDtypeStruct((1, SLOTS), F32),
            jax.ShapeDtypeStruct((1, SLOTS), F32),
        ],
        in_specs=[VMEM] * 4,
        out_specs=[VMEM] * 3,
        compiler_params=params(),
    )(stats, source, reward_of[None, :], length_of[None, :])
    return token_logprobs, advantages.reshape(SLOTS), weighted.reshape(SLOTS)


def solution(mesh):
    finer = Mesh(mesh.devices.reshape(NX, NZ, NY, NC), ("x", "z", "y", "c"))
    every = ("x", "z", "y", "c")
    placed = (P(DP, None, VOCAB), P(None, every), P(DP, None), P(DP, None), P(DP, None), P())

    return jax.shard_map(
        local, mesh=finer, in_specs=placed, out_specs=(P(DP, None), P(DP), P(DP)), check_vma=False
    )
```

```python
import jax
import jax.numpy as jnp
from jax import lax
from jax.experimental import pallas as pl
from jax.experimental.pallas import tpu as pltpu
from jax.sharding import Mesh
from jax.sharding import PartitionSpec as P


SAMPLES = 8
DP = ("x", "z")
VOCAB = ("y", "c")
REWARD_UNIT = 1.0 / 64.0
NX, NZ, NY, NC = 4, 8, 4, 2
SLOTS, WINDOW, WIDTH = 8, 14, 512
HALF = 28
MSG = 32
ROWS = NZ * HALF
META = NZ
SHARD = 501
TALL = ROWS + META
OFFSETS = (0, -1, 1, 2)
F32 = jnp.float32
BF16 = jnp.bfloat16
VMEM = pl.BlockSpec(memory_space=pltpu.VMEM)
SMEM = pl.BlockSpec(memory_space=pltpu.SMEM)
HBM = pl.BlockSpec(memory_space=pltpu.HBM)


def params(mib=32):
    return pltpu.CompilerParams(vmem_limit_bytes=mib * 2**20)


def in_hbm(*arrays):
    return [pltpu.with_memory_space_constraint(a, pltpu.HBM) for a in arrays]


def shift(value, axis, by):
    size = lax.axis_size(axis)
    return lax.ppermute(value, axis, [(i, (i + by) % size) for i in range(size)])


def pack_kernel(hidden_hbm, targets_hbm, lengths_hbm, rewards_hbm, out, hidden, targets, lengths, rewards, sems):
    copies = [
        pltpu.make_async_copy(src, dst, sems.at[k])
        for k, (src, dst) in enumerate(
            (
                (lengths_hbm, lengths),
                (rewards_hbm, rewards),
                (targets_hbm, targets),
                (hidden_hbm, hidden),
            )
        )
    ]
    for copy in copies:
        copy.start()
    for copy in copies:
        copy.wait()
    lane = lax.broadcasted_iota(jnp.int32, (1, 128), 1)
    offsets, both = [], jnp.zeros((1, 128), jnp.int32)
    offset_of = jnp.zeros((MSG, SLOTS), jnp.int32)
    length_of = jnp.zeros((MSG, SLOTS), jnp.int32)
    slot = lax.broadcasted_iota(jnp.int32, (MSG, SLOTS), 1)
    at = jnp.int32(0)
    for g in range(SLOTS):
        offsets.append(at)
        offset_of = jnp.where(slot == g, at, offset_of)
        length_of = jnp.where(slot == g, lengths[0, g], length_of)
        both = jnp.where(lane == g, lengths[0, g], both)
        both = jnp.where(lane == SLOTS + g, rewards[0, g], both)
        at = at + lengths[0, g]
    row_of = lax.broadcasted_iota(jnp.int32, (MSG, SLOTS), 0)
    row = lax.broadcasted_iota(jnp.int32, (MSG, WINDOW), 0)
    step = lax.broadcasted_iota(jnp.int32, (MSG, WINDOW), 1)
    wanted = targets[...]
    digits = [(wanted & 255), (wanted >> 8) & 255, wanted >> 16]
    out_row = lax.broadcasted_iota(jnp.int32, (MSG, WIDTH), 0)
    for half in range(NC):
        rows = jnp.zeros((MSG, WIDTH), F32)
        for t in range(WINDOW):
            here = (row_of + half * HALF == offset_of + t) & (t < length_of) & (row_of < HALF)
            chooser = jnp.where(here, 1.0, 0.0).astype(BF16)
            rows += jnp.dot(chooser, hidden[t], preferred_element_type=F32)
        ids = jnp.zeros((8, MSG), F32)
        for g in range(SLOTS):
            here = (row + half * HALF == offsets[g] + step) & (step < lengths[0, g]) & (row < HALF)
            chooser = jnp.where(here, 1.0, 0.0).astype(BF16)
            three = jnp.concatenate(
                [d[g : g + 1, :] for d in digits] + [jnp.zeros((5, WINDOW), jnp.int32)], axis=0
            )
            ids += lax.dot_general(
                three.astype(F32).astype(BF16),
                chooser,
                (((1,), (1,)), ((), ())),
                preferred_element_type=F32,
            )
        pad = jnp.zeros((1, 128 - MSG), F32)
        meta = jnp.concatenate(
            [ids[0:1], pad, ids[1:2], pad, ids[2:3], pad, both.astype(F32)], axis=1
        )
        message = jnp.where(out_row == HALF, meta, rows).astype(BF16)
        for z in range(NZ):
            out[z * NC + half] = message


def unpack_kernel(got, first, second):
    for core, out in enumerate((first, second)):
        pieces = [got[z * NC + core].astype(F32)[:HALF] for z in range(NZ)]
        if core == 0:
            pieces += [got[z * NC].astype(F32)[HALF : HALF + 1] for z in range(NZ)]
        out[...] = jnp.concatenate(pieces, axis=0).astype(BF16)


def join_kernel(one, two, out):
    out[:ROWS] = one[:ROWS]
    out[ROWS:] = two[:ROWS]


def join(one, two):
    return pl.pallas_call(
        join_kernel,
        out_shape=jax.ShapeDtypeStruct((2 * ROWS, WIDTH), BF16),
        in_specs=[VMEM, VMEM],
        out_specs=VMEM,
        compiler_params=params(),
    )(one, two)


def gathered_planes(own, firsts, lasts):
    both = range(2)
    up = [shift(own[k], firsts[k], 1) for k in both]
    down = [shift(own[k], firsts[k], -1) for k in both]
    far = [shift(up[k], firsts[k], 1) for k in both]
    one, two = [], []
    for k in both:
        one.append(join(own[k], up[k]))
        two.append(join(down[k], far[k]))
    planes = []
    for k in both:
        up1 = shift(one[k], lasts[k], 1)
        down1 = shift(one[k], lasts[k], -1)
        down2 = shift(two[k], lasts[k], -1)
        up2 = shift(two[k], lasts[k], 1)
        far2 = shift(down2, lasts[k], -1)
        far1 = shift(up1, lasts[k], 1)
        planes.append(((one[k], two[k]), (up1, up2), (down1, down2), (far1, far2)))
    return planes, (own[0], up[0], down[0], far[0])


def product(w, block):
    return lax.dot_general(w[...], block, (((1,), (1,)), ((), ())), preferred_element_type=F32)


LOOK = 4


class Arrivals:
    def __init__(self):
        self.order, self.copies, self.begun = [], {}, 0

    def add(self, key, *copies):
        if key not in self.copies:
            self.order.append(key)
            self.copies[key] = copies

    def begin(self, upto):
        while self.begun < min(upto, len(self.order)):
            for copy in self.copies[self.order[self.begun]]:
                copy.start()
            self.begun += 1

    def wait(self, key):
        if self.copies.get(key):
            self.begin(self.order.index(key) + 1 + LOOK)
            for copy in self.copies[key]:
                copy.wait()
            self.copies[key] = ()


def names_of(which):
    return [(k, j, part) for k in range(2) for j in which for part in range(2)]


def plan_of(which):
    plan = []
    for i in [i for i in range(NX) if i not in which] + list(which):
        terms = [((j, 0), (0, j, i // 2), i % 2 * ROWS) for j in which]
        if i in which:
            terms += [((j, 1), (1, i, j // 2), j % 2 * ROWS) for j in range(NY)]
        plan.append((i, terms))
    return plan


LOCAL, NEAR, FAR = (0,), (1, 2), (3,)
KEPT = tuple((j, 1) for j in range(NY)) + tuple((j, 0) for j in NEAR + FAR)
NEAR_LATE = [n for n in names_of(NEAR) if n[1] - 1 != n[2] or n == (1, 2, 1)]


def piece_copies(arrivals, name, pieces, late, held_p, sems):
    ref = pieces[name]
    if name not in late:
        return ref
    n = late.index(name)
    arrivals.add(name, pltpu.make_async_copy(ref, held_p.at[n, pl.ds(0, ref.shape[0])], sems.at[n]))
    return held_p.at[n]


def local_kernel(at, *refs):
    pieces = dict(zip(names_of(LOCAL), refs))
    weights, rest = refs[len(pieces) : len(pieces) + 2], refs[len(pieces) + 2 :]
    acc, kept, held_w, sems_w = rest
    arrivals, slices = Arrivals(), {}

    def slice_copies(key):
        j, colour = key
        slices[key] = kept.at[KEPT.index(key)] if key in KEPT else held_w
        column = ((at[0] + OFFSETS[j] + NY) % NY * NC + colour) * WIDTH
        column = pl.multiple_of(column, WIDTH)
        arrivals.add(
            key,
            *(
                pltpu.make_async_copy(
                    weights[w].at[:, pl.ds(column, WIDTH)], slices[key].at[w], sems_w.at[j, colour, w]
                )
                for w in range(2)
            ),
        )

    plan = plan_of(LOCAL)
    for _, terms in plan:
        for key, _, _ in terms:
            if key not in slices:
                slice_copies(key)
    for key in KEPT:
        if key not in slices:
            slice_copies(key)
    arrivals.begin(LOOK)
    for i, terms in plan:
        total = [None, None]
        for key, name, lo in terms:
            arrivals.wait(key)
            for w in range(2):
                term = product(slices[key].at[w], pieces[name][lo : lo + ROWS, :])
                total[w] = term if total[w] is None else total[w] + term
        for w in range(2):
            acc[i, w] = total[w]
    for key in KEPT:
        arrivals.wait(key)


def add_terms(which, before, kept, views, acc, ready):
    for i, terms in plan_of(which):
        total = [before[i, w] for w in range(2)]
        for key, name, lo in terms:
            ready(name)
            for w in range(2):
                total[w] = total[w] + product(kept.at[KEPT.index(key), w], views[name][lo : lo + ROWS, :])
        for w in range(2):
            acc[i, w] = total[w]


def near_kernel(*refs):
    pieces = dict(zip(names_of(NEAR), refs))
    before, kept, acc, held_p, sems = refs[len(pieces) :]
    arrivals, views = Arrivals(), {}
    for _, terms in plan_of(NEAR):
        for _, name, _ in terms:
            if name not in views:
                views[name] = piece_copies(arrivals, name, pieces, NEAR_LATE, held_p, sems)
    arrivals.begin(LOOK)
    add_terms(NEAR, before, kept, views, acc, arrivals.wait)


def far_kernel(at, *refs):
    pieces = dict(zip(names_of(FAR), refs))
    before, kept, ids, out, acc, held = refs[len(pieces) :]
    add_terms(FAR, before, kept, pieces, acc, lambda name: None)
    statistics(at, ids, acc, out, held)


def statistics(at, ids, acc, out, held):
    x = at[1]
    held[...] = jnp.zeros_like(held)
    column = lax.broadcasted_iota(jnp.int32, (SHARD, ROWS), 0)
    for i in range(NX):
        own, other = acc[i, 0], acc[i, 1]
        top = jnp.maximum(jnp.max(own, 0, keepdims=True), jnp.max(other, 0, keepdims=True))
        total = jnp.sum(jnp.exp(own - top), 0, keepdims=True) + jnp.sum(
            jnp.exp(other - top), 0, keepdims=True
        )
        wanted = ids[i : i + 1, :ROWS]
        hit = jnp.sum(jnp.where(column == wanted - at[2], own, 0.0), 0, keepdims=True)
        hit += jnp.sum(jnp.where(column == wanted - at[3], other, 0.0), 0, keepdims=True)
        x_at = (x + OFFSETS[i] + NX) % NX
        held[pl.ds(x_at, 1), :ROWS] = top + jnp.log(total)
        held[pl.ds(4 + x_at, 1), :ROWS] = hit
    for k in range(out.shape[0]):
        out[k] = held[...]


def head(at, planes, weights, ids):
    acc = pltpu.VMEM((NX, 2, SHARD, ROWS), F32)
    kept = pltpu.VMEM((len(KEPT), 2, SHARD, WIDTH), BF16)

    def operands(which, late=()):
        parts, specs = [], []
        for name in names_of(which):
            piece = planes[name[0]][name[1]][name[2]]
            parts += in_hbm(piece) if name in late else [piece]
            specs.append(HBM if name in late else VMEM)
        return parts, specs

    parts, specs = operands(LOCAL)
    sums, slices = pl.pallas_call(
        local_kernel,
        out_shape=[acc, kept],
        in_specs=[SMEM] + specs + [HBM] * 2,
        out_specs=[VMEM, VMEM],
        scratch_shapes=[pltpu.VMEM((2, SHARD, WIDTH), BF16), pltpu.SemaphoreType.DMA((NY, NC, 2))],
        compiler_params=params(20),
    )(at, *parts, *weights)
    parts, specs = operands(NEAR, NEAR_LATE)
    sums = pl.pallas_call(
        near_kernel,
        out_shape=acc,
        in_specs=specs + [VMEM] * 2,
        out_specs=VMEM,
        scratch_shapes=[
            pltpu.VMEM((len(NEAR_LATE), 2 * ROWS, WIDTH), BF16),
            pltpu.SemaphoreType.DMA((len(NEAR_LATE),)),
        ],
        input_output_aliases={len(parts): 0},
        compiler_params=params(20),
    )(*parts, sums, slices)
    parts, specs = operands(FAR)
    return pl.pallas_call(
        far_kernel,
        out_shape=jax.ShapeDtypeStruct((NX * NY, 8, 256), F32),
        in_specs=[SMEM] + specs + [VMEM] * 3,
        out_specs=VMEM,
        scratch_shapes=[acc, pltpu.VMEM((8, 256), F32)],
        compiler_params=params(24),
    )(at, *parts, sums, slices, ids)


def merged_parts(parts):
    top, hit = parts[0][:4], parts[0][4:]
    for part in parts[1:]:
        top = jnp.maximum(top, part[:4])
        hit = hit + part[4:]
    total = jnp.zeros_like(top)
    for part in parts:
        total = total + jnp.exp(part[:4] - top)
    return top + jnp.log(total), hit


def merge_kernel(parts, out):
    lse, hit = merged_parts([parts[k] for k in range(parts.shape[0])])
    for k in range(out.shape[0]):
        out[k, :4] = lse
        out[k, 4:] = hit


def final_kernel(parts, source, reward, length, logprobs, advantage, weighted):
    tables = []
    for core in range(NC):
        lse, hit = merged_parts([parts[z * NC + core] for z in range(NZ)])
        tables.append(hit - lse)
    lane = lax.broadcasted_iota(jnp.int32, (SLOTS, 256), 1)
    wanted = source[...]
    total = jnp.zeros((SLOTS, 1), F32)
    columns = []
    for t in range(WINDOW):
        at = wanted[:, t : t + 1]
        found = jnp.zeros((SLOTS, 256), F32)
        for core in range(NC):
            for x in range(NX):
                here = at - (core * NX + x) * 256 == lane
                found = jnp.where(here, tables[core][x : x + 1, :], found)
        value = jnp.sum(found, axis=1, keepdims=True)
        columns.append(value)
        total = total + value
    logprobs[...] = jnp.concatenate(columns, axis=1)
    row = lax.broadcasted_iota(jnp.int32, (SLOTS, SLOTS), 0)
    across = lax.broadcasted_iota(jnp.int32, (SLOTS, SLOTS), 1)
    line = jnp.sum(jnp.where(row == across, total, 0.0), axis=0, keepdims=True)
    own = reward[...].astype(F32) * REWARD_UNIT
    spare = own - (jnp.sum(own, axis=1, keepdims=True) - own) / (SAMPLES - 1.0)
    advantage[...] = spare
    weighted[...] = spare * line / length[...].astype(F32)


def local(hidden, weight, targets, lengths, rewards, arrival):
    shard = weight.shape[1]
    x, z, y, c = (lax.axis_index(a) for a in ("x", "z", "y", "c"))
    swapped = shift(weight, "c", 1)
    sent = pl.pallas_call(
        pack_kernel,
        out_shape=pltpu.VMEM((NZ * NC, MSG, WIDTH), BF16),
        in_specs=[HBM] * 4,
        out_specs=VMEM,
        scratch_shapes=[
            pltpu.VMEM((WINDOW, SLOTS, WIDTH), BF16),
            pltpu.VMEM((SLOTS, WINDOW), jnp.int32),
            pltpu.SMEM((1, SLOTS), jnp.int32),
            pltpu.SMEM((1, SLOTS), jnp.int32),
            pltpu.SemaphoreType.DMA((4,)),
        ],
        compiler_params=params(),
    )(*in_hbm(hidden.transpose(1, 0, 2), targets, lengths, rewards))
    got = lax.all_to_all(sent, ("z", "c"), 0, 0, tiled=True)
    own0, own1 = pl.pallas_call(
        unpack_kernel,
        out_shape=[
            jax.ShapeDtypeStruct((TALL, WIDTH), BF16),
            jax.ShapeDtypeStruct((ROWS, WIDTH), BF16),
        ],
        in_specs=[VMEM],
        out_specs=[VMEM, VMEM],
        compiler_params=params(),
    )(got)
    planes, line0 = gathered_planes((own0, own1), ("x", "y"), ("y", "x"))
    metas = jnp.stack([block[ROWS:] for block in line0])
    whole = metas.astype(F32).astype(jnp.int32)
    ids = whole[:, :, :HALF] + 256 * whole[:, :, 128 : 128 + HALF] + 65536 * whole[:, :, 256 : 256 + HALF]
    ids = jnp.pad(ids.reshape(NX, ROWS), ((0, 4), (0, 0)), constant_values=-1)

    dp = x * NZ + z
    base = (dp * NY + y) * NC
    at = jnp.stack([y, x, (base + c) * shard, (base + 1 - c) * shard]).astype(jnp.int32)

    order = (lax.iota(jnp.int32, NX) - x + NX) % NX
    relative = jnp.where(order == 0, 0, jnp.where(order == 3, 1, order + 1))
    per_slot = jnp.sum(
        jnp.where(
            (relative[:, None] == lax.iota(jnp.int32, NX)[None, :])[:, :, None, None],
            whole[None, :, :, 384 : 384 + 2 * SLOTS],
            0,
        ),
        axis=1,
    ).reshape(NX * NZ, 2 * SLOTS)
    all_lengths, all_rewards = per_slot[:, :SLOTS], per_slot[:, SLOTS:]
    count = NX * NZ * SLOTS
    slot_ids = lax.iota(jnp.int32, count)
    mine = lax.iota(jnp.int32, SLOTS) + dp * SLOTS
    matching = arrival[None, :] == mine[:, None]

    def lookup(table):
        return jnp.sum(jnp.where(matching, table.reshape(count)[None, :], 0), axis=1)

    slot_of = lookup(slot_ids)
    length_of = lookup(all_lengths)
    reward_of = lookup(all_rewards)
    offset_of = lookup(jnp.cumsum(all_lengths, axis=1) - all_lengths)
    group = slot_of // SLOTS
    line = offset_of[:, None] + lax.iota(jnp.int32, WINDOW)[None, :]
    usable = lax.iota(jnp.int32, WINDOW)[None, :] < length_of[:, None]
    place = group // NZ * 256 + group % NZ * HALF
    source = jnp.where(usable, place[:, None] + line // HALF * 1024 + line % HALF, -1)

    partial = head(at, planes, in_hbm(weight.T, swapped.T), ids)

    stats = lax.all_to_all(partial, ("x", "y"), 0, 0, tiled=True)
    stats = pl.pallas_call(
        merge_kernel,
        out_shape=pltpu.VMEM((NZ * NC, 8, 256), F32),
        in_specs=[VMEM],
        out_specs=VMEM,
        compiler_params=params(),
    )(stats)
    stats = lax.all_to_all(stats, ("z", "c"), 0, 0, tiled=True)
    token_logprobs, advantages, weighted = pl.pallas_call(
        final_kernel,
        out_shape=[
            jax.ShapeDtypeStruct((SLOTS, WINDOW), F32),
            jax.ShapeDtypeStruct((1, SLOTS), F32),
            jax.ShapeDtypeStruct((1, SLOTS), F32),
        ],
        in_specs=[VMEM] * 4,
        out_specs=[VMEM] * 3,
        compiler_params=params(),
    )(stats, source, reward_of[None, :], length_of[None, :])
    return token_logprobs, advantages.reshape(SLOTS), weighted.reshape(SLOTS)


def solution(mesh):
    finer = Mesh(mesh.devices.reshape(NX, NZ, NY, NC), ("x", "z", "y", "c"))
    every = ("x", "z", "y", "c")
    placed = (P(DP, None, VOCAB), P(None, every), P(DP, None), P(DP, None), P(DP, None), P())

    return jax.shard_map(
        local, mesh=finer, in_specs=placed, out_specs=(P(DP, None), P(DP), P(DP)), check_vma=False
    )
```

```python
import jax
import jax.numpy as jnp
from jax import lax
from jax.experimental import pallas as pl
from jax.experimental.pallas import tpu as pltpu
from jax.sharding import Mesh
from jax.sharding import PartitionSpec as P


SAMPLES = 8
DP = ("x", "z")
VOCAB = ("y", "c")
REWARD_UNIT = 1.0 / 64.0
NX, NZ, NY, NC = 4, 8, 4, 2
SLOTS, WINDOW, WIDTH = 8, 14, 512
HALF = 28
MSG = 32
ROWS = NZ * HALF
META = NZ
SHARD = 501
TALL = ROWS + META
OFFSETS = (0, -1, 1, 2)
F32 = jnp.float32
BF16 = jnp.bfloat16
VMEM = pl.BlockSpec(memory_space=pltpu.VMEM)
SMEM = pl.BlockSpec(memory_space=pltpu.SMEM)
HBM = pl.BlockSpec(memory_space=pltpu.HBM)


def params(mib=32):
    return pltpu.CompilerParams(vmem_limit_bytes=mib * 2**20)


def in_hbm(*arrays):
    return [pltpu.with_memory_space_constraint(a, pltpu.HBM) for a in arrays]


def shift(value, axis, by):
    size = lax.axis_size(axis)
    return lax.ppermute(value, axis, [(i, (i + by) % size) for i in range(size)])


def pack_kernel(hidden_hbm, targets_hbm, lengths_hbm, rewards_hbm, out, hidden, targets, lengths, rewards, sems):
    copies = [
        pltpu.make_async_copy(src, dst, sems.at[k])
        for k, (src, dst) in enumerate(
            (
                (lengths_hbm, lengths),
                (rewards_hbm, rewards),
                (targets_hbm, targets),
                (hidden_hbm, hidden),
            )
        )
    ]
    for copy in copies:
        copy.start()
    for copy in copies:
        copy.wait()
    lane = lax.broadcasted_iota(jnp.int32, (1, 128), 1)
    offsets, both = [], jnp.zeros((1, 128), jnp.int32)
    offset_of = jnp.zeros((MSG, SLOTS), jnp.int32)
    length_of = jnp.zeros((MSG, SLOTS), jnp.int32)
    slot = lax.broadcasted_iota(jnp.int32, (MSG, SLOTS), 1)
    at = jnp.int32(0)
    for g in range(SLOTS):
        offsets.append(at)
        offset_of = jnp.where(slot == g, at, offset_of)
        length_of = jnp.where(slot == g, lengths[0, g], length_of)
        both = jnp.where(lane == g, lengths[0, g], both)
        both = jnp.where(lane == SLOTS + g, rewards[0, g], both)
        at = at + lengths[0, g]
    row_of = lax.broadcasted_iota(jnp.int32, (MSG, SLOTS), 0)
    row = lax.broadcasted_iota(jnp.int32, (MSG, WINDOW), 0)
    step = lax.broadcasted_iota(jnp.int32, (MSG, WINDOW), 1)
    wanted = targets[...]
    digits = [(wanted & 255), (wanted >> 8) & 255, wanted >> 16]
    out_row = lax.broadcasted_iota(jnp.int32, (MSG, WIDTH), 0)
    for half in range(NC):
        rows = jnp.zeros((MSG, WIDTH), F32)
        for t in range(WINDOW):
            here = (row_of + half * HALF == offset_of + t) & (t < length_of) & (row_of < HALF)
            chooser = jnp.where(here, 1.0, 0.0).astype(BF16)
            rows += jnp.dot(chooser, hidden[t], preferred_element_type=F32)
        ids = jnp.zeros((8, MSG), F32)
        for g in range(SLOTS):
            here = (row + half * HALF == offsets[g] + step) & (step < lengths[0, g]) & (row < HALF)
            chooser = jnp.where(here, 1.0, 0.0).astype(BF16)
            three = jnp.concatenate(
                [d[g : g + 1, :] for d in digits] + [jnp.zeros((5, WINDOW), jnp.int32)], axis=0
            )
            ids += lax.dot_general(
                three.astype(F32).astype(BF16),
                chooser,
                (((1,), (1,)), ((), ())),
                preferred_element_type=F32,
            )
        pad = jnp.zeros((1, 128 - MSG), F32)
        meta = jnp.concatenate(
            [ids[0:1], pad, ids[1:2], pad, ids[2:3], pad, both.astype(F32)], axis=1
        )
        message = jnp.where(out_row == HALF, meta, rows).astype(BF16)
        for z in range(NZ):
            out[z * NC + half] = message


def unpack_kernel(got, first, second):
    for core, out in enumerate((first, second)):
        pieces = [got[z * NC + core].astype(F32)[:HALF] for z in range(NZ)]
        if core == 0:
            pieces += [got[z * NC].astype(F32)[HALF : HALF + 1] for z in range(NZ)]
        out[...] = jnp.concatenate(pieces, axis=0).astype(BF16)


def join_kernel(one, two, out):
    out[:ROWS] = one[:ROWS]
    out[ROWS:] = two[:ROWS]


def join(one, two):
    return pl.pallas_call(
        join_kernel,
        out_shape=jax.ShapeDtypeStruct((2 * ROWS, WIDTH), BF16),
        in_specs=[VMEM, VMEM],
        out_specs=VMEM,
        compiler_params=params(),
    )(one, two)


def gathered_planes(own, firsts, lasts):
    both = range(2)
    up = [shift(own[k], firsts[k], 1) for k in both]
    down = [shift(own[k], firsts[k], -1) for k in both]
    far = [shift(up[k], firsts[k], 1) for k in both]
    one, two = [], []
    for k in both:
        one.append(join(own[k], up[k]))
        two.append(join(down[k], far[k]))
    planes = []
    for k in both:
        up1 = shift(one[k], lasts[k], 1)
        down1 = shift(one[k], lasts[k], -1)
        down2 = shift(two[k], lasts[k], -1)
        up2 = shift(two[k], lasts[k], 1)
        far2 = shift(down2, lasts[k], -1)
        far1 = shift(up1, lasts[k], 1)
        planes.append(((one[k], two[k]), (up1, up2), (down1, down2), (far1, far2)))
    return planes, (own[0], up[0], down[0], far[0])


def product(w, block):
    return lax.dot_general(w[...], block, (((1,), (1,)), ((), ())), preferred_element_type=F32)


LOOK = 4


class Arrivals:
    def __init__(self):
        self.order, self.copies, self.begun = [], {}, 0

    def add(self, key, *copies):
        if key not in self.copies:
            self.order.append(key)
            self.copies[key] = copies

    def begin(self, upto):
        while self.begun < min(upto, len(self.order)):
            for copy in self.copies[self.order[self.begun]]:
                copy.start()
            self.begun += 1

    def wait(self, key):
        if self.copies.get(key):
            self.begin(self.order.index(key) + 1 + LOOK)
            for copy in self.copies[key]:
                copy.wait()
            self.copies[key] = ()


def names_of(which):
    return [(k, j, part) for k in range(2) for j in which for part in range(2)]


def plan_of(which):
    plan = []
    for i in [i for i in range(NX) if i not in which] + list(which):
        terms = [((j, 0), (0, j, i // 2), i % 2 * ROWS) for j in which]
        if i in which:
            terms += [((j, 1), (1, i, j // 2), j % 2 * ROWS) for j in range(NY)]
        plan.append((i, terms))
    return plan


LOCAL, NEAR, FAR = (0,), (1, 2), (3,)
KEPT = tuple((j, 1) for j in range(NY)) + tuple((j, 0) for j in NEAR + FAR)
NEAR_LATE = [n for n in names_of(NEAR) if n[1] - 1 != n[2] or n == (1, 2, 1)]


def piece_copies(arrivals, name, pieces, late, held_p, sems):
    ref = pieces[name]
    if name not in late:
        return ref
    n = late.index(name)
    arrivals.add(name, pltpu.make_async_copy(ref, held_p.at[n, pl.ds(0, ref.shape[0])], sems.at[n]))
    return held_p.at[n]


def local_kernel(at, *refs):
    pieces = dict(zip(names_of(LOCAL), refs))
    weights, rest = refs[len(pieces) : len(pieces) + 2], refs[len(pieces) + 2 :]
    acc, kept, held_w, sems_w = rest
    arrivals, slices = Arrivals(), {}

    def slice_copies(key):
        j, colour = key
        slices[key] = kept.at[KEPT.index(key)] if key in KEPT else held_w
        column = ((at[0] + OFFSETS[j] + NY) % NY * NC + colour) * WIDTH
        column = pl.multiple_of(column, WIDTH)
        arrivals.add(
            key,
            *(
                pltpu.make_async_copy(
                    weights[w].at[:, pl.ds(column, WIDTH)], slices[key].at[w], sems_w.at[j, colour, w]
                )
                for w in range(2)
            ),
        )

    plan = plan_of(LOCAL)
    for _, terms in plan:
        for key, _, _ in terms:
            if key not in slices:
                slice_copies(key)
    for key in KEPT:
        if key not in slices:
            slice_copies(key)
    arrivals.begin(LOOK)
    for i, terms in plan:
        total = [None, None]
        for key, name, lo in terms:
            arrivals.wait(key)
            for w in range(2):
                term = product(slices[key].at[w], pieces[name][lo : lo + ROWS, :])
                total[w] = term if total[w] is None else total[w] + term
        for w in range(2):
            acc[i, w] = total[w]
    for key in KEPT:
        arrivals.wait(key)


def add_terms(which, before, kept, views, acc, ready):
    for i, terms in plan_of(which):
        total = [before[i, w] for w in range(2)]
        for key, name, lo in terms:
            ready(name)
            for w in range(2):
                total[w] = total[w] + product(kept.at[KEPT.index(key), w], views[name][lo : lo + ROWS, :])
        for w in range(2):
            acc[i, w] = total[w]


def near_kernel(*refs):
    pieces = dict(zip(names_of(NEAR), refs))
    before, kept, acc, held_p, sems = refs[len(pieces) :]
    arrivals, views = Arrivals(), {}
    for _, terms in plan_of(NEAR):
        for _, name, _ in terms:
            if name not in views:
                views[name] = piece_copies(arrivals, name, pieces, NEAR_LATE, held_p, sems)
    arrivals.begin(LOOK)
    add_terms(NEAR, before, kept, views, acc, arrivals.wait)


def far_kernel(at, *refs):
    pieces = dict(zip(names_of(FAR), refs))
    before, kept, ids, out, acc, held = refs[len(pieces) :]
    add_terms(FAR, before, kept, pieces, acc, lambda name: None)
    statistics(at, ids, acc, out, held)


def statistics(at, ids, acc, out, held):
    x = at[1]
    whole = SHARD // 8 * 8
    held[...] = jnp.zeros_like(held)
    row = lax.broadcasted_iota(jnp.int32, (8, ROWS), 0)
    rest_row = lax.broadcasted_iota(jnp.int32, (SHARD - whole, ROWS), 0)
    for i in range(NX):
        top = acc[i, 0, :8]
        for w in range(2):
            for r in range(0, whole, 8):
                top = jnp.maximum(top, acc[i, w, r : r + 8])
        top = jnp.max(top, 0, keepdims=True)
        for w in range(2):
            top = jnp.maximum(top, jnp.max(acc[i, w, whole:], 0, keepdims=True))
        total, hit = jnp.zeros((8, ROWS), F32), jnp.zeros((8, ROWS), F32)
        rest_total, rest_hit = jnp.zeros((1, ROWS), F32), jnp.zeros((1, ROWS), F32)
        for w in range(2):
            wanted = ids[i : i + 1, :ROWS] - at[2 + w]
            column = wanted - row
            for r in range(0, whole, 8):
                value = acc[i, w, r : r + 8]
                total = total + jnp.exp(value - top)
                hit = jnp.where(column == r, value, hit)
            value = acc[i, w, whole:]
            rest_total += jnp.sum(jnp.exp(value - top), 0, keepdims=True)
            here = wanted - rest_row == whole
            rest_hit += jnp.sum(jnp.where(here, value, 0.0), 0, keepdims=True)
        x_at = (x + OFFSETS[i] + NX) % NX
        total = jnp.sum(total, 0, keepdims=True) + rest_total
        held[pl.ds(x_at, 1), :ROWS] = top + jnp.log(total)
        held[pl.ds(4 + x_at, 1), :ROWS] = jnp.sum(hit, 0, keepdims=True) + rest_hit
    for k in range(out.shape[0]):
        out[k] = held[...]


def head(at, planes, weights, ids):
    acc = pltpu.VMEM((NX, 2, SHARD, ROWS), F32)
    kept = pltpu.VMEM((len(KEPT), 2, SHARD, WIDTH), BF16)

    def operands(which, late=()):
        parts, specs = [], []
        for name in names_of(which):
            piece = planes[name[0]][name[1]][name[2]]
            parts += in_hbm(piece) if name in late else [piece]
            specs.append(HBM if name in late else VMEM)
        return parts, specs

    parts, specs = operands(LOCAL)
    sums, slices = pl.pallas_call(
        local_kernel,
        out_shape=[acc, kept],
        in_specs=[SMEM] + specs + [HBM] * 2,
        out_specs=[VMEM, VMEM],
        scratch_shapes=[pltpu.VMEM((2, SHARD, WIDTH), BF16), pltpu.SemaphoreType.DMA((NY, NC, 2))],
        compiler_params=params(20),
    )(at, *parts, *weights)
    parts, specs = operands(NEAR, NEAR_LATE)
    sums = pl.pallas_call(
        near_kernel,
        out_shape=acc,
        in_specs=specs + [VMEM] * 2,
        out_specs=VMEM,
        scratch_shapes=[
            pltpu.VMEM((len(NEAR_LATE), 2 * ROWS, WIDTH), BF16),
            pltpu.SemaphoreType.DMA((len(NEAR_LATE),)),
        ],
        input_output_aliases={len(parts): 0},
        compiler_params=params(20),
    )(*parts, sums, slices)
    parts, specs = operands(FAR)
    return pl.pallas_call(
        far_kernel,
        out_shape=jax.ShapeDtypeStruct((NX * NY, 8, 256), F32),
        in_specs=[SMEM] + specs + [VMEM] * 3,
        out_specs=VMEM,
        scratch_shapes=[acc, pltpu.VMEM((8, 256), F32)],
        compiler_params=params(24),
    )(at, *parts, sums, slices, ids)


def merged_parts(parts):
    top, hit = parts[0][:4], parts[0][4:]
    for part in parts[1:]:
        top = jnp.maximum(top, part[:4])
        hit = hit + part[4:]
    total = jnp.zeros_like(top)
    for part in parts:
        total = total + jnp.exp(part[:4] - top)
    return top + jnp.log(total), hit


def merge_kernel(parts, out):
    lse, hit = merged_parts([parts[k] for k in range(parts.shape[0])])
    for k in range(out.shape[0]):
        out[k, :4] = lse
        out[k, 4:] = hit


def final_kernel(parts, source, reward, length, logprobs, advantage, weighted):
    tables = []
    for core in range(NC):
        lse, hit = merged_parts([parts[z * NC + core] for z in range(NZ)])
        tables.append(hit - lse)
    lane = lax.broadcasted_iota(jnp.int32, (SLOTS, 256), 1)
    wanted = source[...]
    total = jnp.zeros((SLOTS, 1), F32)
    columns = []
    for t in range(WINDOW):
        at = wanted[:, t : t + 1]
        found = jnp.zeros((SLOTS, 256), F32)
        for core in range(NC):
            for x in range(NX):
                here = at - (core * NX + x) * 256 == lane
                found = jnp.where(here, tables[core][x : x + 1, :], found)
        value = jnp.sum(found, axis=1, keepdims=True)
        columns.append(value)
        total = total + value
    logprobs[...] = jnp.concatenate(columns, axis=1)
    row = lax.broadcasted_iota(jnp.int32, (SLOTS, SLOTS), 0)
    across = lax.broadcasted_iota(jnp.int32, (SLOTS, SLOTS), 1)
    line = jnp.sum(jnp.where(row == across, total, 0.0), axis=0, keepdims=True)
    own = reward[...].astype(F32) * REWARD_UNIT
    spare = own - (jnp.sum(own, axis=1, keepdims=True) - own) / (SAMPLES - 1.0)
    advantage[...] = spare
    weighted[...] = spare * line / length[...].astype(F32)


def local(hidden, weight, targets, lengths, rewards, arrival):
    shard = weight.shape[1]
    x, z, y, c = (lax.axis_index(a) for a in ("x", "z", "y", "c"))
    swapped = shift(weight, "c", 1)
    sent = pl.pallas_call(
        pack_kernel,
        out_shape=pltpu.VMEM((NZ * NC, MSG, WIDTH), BF16),
        in_specs=[HBM] * 4,
        out_specs=VMEM,
        scratch_shapes=[
            pltpu.VMEM((WINDOW, SLOTS, WIDTH), BF16),
            pltpu.VMEM((SLOTS, WINDOW), jnp.int32),
            pltpu.SMEM((1, SLOTS), jnp.int32),
            pltpu.SMEM((1, SLOTS), jnp.int32),
            pltpu.SemaphoreType.DMA((4,)),
        ],
        compiler_params=params(),
    )(*in_hbm(hidden.transpose(1, 0, 2), targets, lengths, rewards))
    got = lax.all_to_all(sent, ("z", "c"), 0, 0, tiled=True)
    own0, own1 = pl.pallas_call(
        unpack_kernel,
        out_shape=[
            jax.ShapeDtypeStruct((TALL, WIDTH), BF16),
            jax.ShapeDtypeStruct((ROWS, WIDTH), BF16),
        ],
        in_specs=[VMEM],
        out_specs=[VMEM, VMEM],
        compiler_params=params(),
    )(got)
    planes, line0 = gathered_planes((own0, own1), ("x", "y"), ("y", "x"))
    metas = jnp.stack([block[ROWS:] for block in line0])
    whole = metas.astype(F32).astype(jnp.int32)
    ids = whole[:, :, :HALF] + 256 * whole[:, :, 128 : 128 + HALF] + 65536 * whole[:, :, 256 : 256 + HALF]
    ids = jnp.pad(ids.reshape(NX, ROWS), ((0, 4), (0, 0)), constant_values=-1)

    dp = x * NZ + z
    base = (dp * NY + y) * NC
    at = jnp.stack([y, x, (base + c) * shard, (base + 1 - c) * shard]).astype(jnp.int32)

    order = (lax.iota(jnp.int32, NX) - x + NX) % NX
    relative = jnp.where(order == 0, 0, jnp.where(order == 3, 1, order + 1))
    per_slot = jnp.sum(
        jnp.where(
            (relative[:, None] == lax.iota(jnp.int32, NX)[None, :])[:, :, None, None],
            whole[None, :, :, 384 : 384 + 2 * SLOTS],
            0,
        ),
        axis=1,
    ).reshape(NX * NZ, 2 * SLOTS)
    all_lengths, all_rewards = per_slot[:, :SLOTS], per_slot[:, SLOTS:]
    count = NX * NZ * SLOTS
    slot_ids = lax.iota(jnp.int32, count)
    mine = lax.iota(jnp.int32, SLOTS) + dp * SLOTS
    matching = arrival[None, :] == mine[:, None]

    def lookup(table):
        return jnp.sum(jnp.where(matching, table.reshape(count)[None, :], 0), axis=1)

    slot_of = lookup(slot_ids)
    length_of = lookup(all_lengths)
    reward_of = lookup(all_rewards)
    offset_of = lookup(jnp.cumsum(all_lengths, axis=1) - all_lengths)
    group = slot_of // SLOTS
    line = offset_of[:, None] + lax.iota(jnp.int32, WINDOW)[None, :]
    usable = lax.iota(jnp.int32, WINDOW)[None, :] < length_of[:, None]
    place = group // NZ * 256 + group % NZ * HALF
    source = jnp.where(usable, place[:, None] + line // HALF * 1024 + line % HALF, -1)

    partial = head(at, planes, in_hbm(weight.T, swapped.T), ids)

    stats = lax.all_to_all(partial, ("x", "y"), 0, 0, tiled=True)
    stats = pl.pallas_call(
        merge_kernel,
        out_shape=pltpu.VMEM((NZ * NC, 8, 256), F32),
        in_specs=[VMEM],
        out_specs=VMEM,
        compiler_params=params(),
    )(stats)
    stats = lax.all_to_all(stats, ("z", "c"), 0, 0, tiled=True)
    token_logprobs, advantages, weighted = pl.pallas_call(
        final_kernel,
        out_shape=[
            jax.ShapeDtypeStruct((SLOTS, WINDOW), F32),
            jax.ShapeDtypeStruct((1, SLOTS), F32),
            jax.ShapeDtypeStruct((1, SLOTS), F32),
        ],
        in_specs=[VMEM] * 4,
        out_specs=[VMEM] * 3,
        compiler_params=params(),
    )(stats, source, reward_of[None, :], length_of[None, :])
    return token_logprobs, advantages.reshape(SLOTS), weighted.reshape(SLOTS)


def solution(mesh):
    finer = Mesh(mesh.devices.reshape(NX, NZ, NY, NC), ("x", "z", "y", "c"))
    every = ("x", "z", "y", "c")
    placed = (P(DP, None, VOCAB), P(None, every), P(DP, None), P(DP, None), P(DP, None), P())

    return jax.shard_map(
        local, mesh=finer, in_specs=placed, out_specs=(P(DP, None), P(DP), P(DP)), check_vma=False
    )
```
